128 devices in a mesh: rep: 8 (over y_lo, z), inst: 16 (over y_hi, x, core).
Axes of the slice: x: 4, y: 4 (y_hi: 2, y_lo: 2; y = y_hi * 2 + y_lo), z: 4, core: 2. Of those that a mesh axis runs over, the one named last changes fastest.
Arguments:
- acts: bfloat16 [131072, 4096], P(('rep', 'inst')), may hold values from -6 to 6
- grad_keys: bfloat16 [131072, 1024], P(('rep', 'inst')), may hold values from -0.03125 to 0.03125
- grad_values: bfloat16 [131072, 1024], P(('rep', 'inst')), may hold values from -0.03125 to 0.03125
- grad_logits: bfloat16 [8, 131072], P(None, ('rep', 'inst')), may hold values from -0.03125 to 0.03125
- order: int32 [32], replicated, may hold values from 0 to 31, each once
- bucket_param: float32 [4, 2048, 1024], P(None, 'inst'), may hold values from -6 to 6
- bucket_m: float32 [4, 2048, 1024], P(None, 'inst'), may hold values from -6 to 6
- bucket_v: float32 [4, 2048, 1024], P(None, 'inst'), may hold values from 0.25 to 4
- router_param: float32 [32, 1024], P('inst'), may hold values from -6 to 6
- router_m: float32 [32, 1024], P('inst'), may hold values from -6 to 6
- router_v: float32 [32, 1024], P('inst'), may hold values from 0.25 to 4
Outputs:
- new_param: float32 [4, 2048, 1024], P(None, 'inst')
- new_moment: float32 [4, 2048, 1024], P(None, 'inst')
- new_second: float32 [4, 2048, 1024], P(None, 'inst')
- router_new_param: float32 [32, 1024], P('inst')
- router_new_moment: float32 [32, 1024], P('inst')
- router_new_second: float32 [32, 1024], P('inst')
The draws below stay inside these ranges and needn't reach their ends.
Inputs may be any that keep to these rules, and one draw needn't show every extreme that they name: order is a permutation of the 32 row blocks; entries with k * 8 <= s < (k + 1) * 8 fill bucket k.
All inputs are finite; a program needn't handle non-finite values.
Results may differ from the reference program's by a relative error of at most 0.0003.
Values sent between devices are 32-bit elements; how exact they have to be, the bound alone decides.
A program may use at most 256 MiB of HBM per device.

```python
import math
import jax
import jax.numpy as jnp
from jax import lax

D = 4096
KV = 1024
EXPERTS = 8
BUCKETS = 4
BLOCK_ROWS = 256
TOKENS = 131072
BLOCKS = 32
BUCKET_ROWS = 2048
ROUTER_ROWS = 32


def levels(rng, extent, split, least, high):
    factor_of, own = 1.0, jax.random.fold_in(rng, 6)
    for axis_at, parts in split:
        steps = jnp.exp(jax.random.uniform(jax.random.fold_in(own, axis_at), (parts,), jnp.float32, least / len(split), high / len(split)))
        factor_of = factor_of * jnp.repeat(steps, extent[axis_at] // parts).reshape([-1 if axis == axis_at else 1 for axis in range(len(extent))])
    return factor_of


def centred(own_key, dims, spread, most, shards=(), dtype=jnp.bfloat16):
    entries = spread * jax.random.normal(own_key, dims, jnp.float32)
    if shards:
        entries = entries * levels(own_key, dims, shards, -0.22, 0.18)
    return jnp.clip(entries, -most, most).astype(dtype)


def setup_inputs(seed: int = 0) -> dict:
    arg_keys = jax.random.split(jax.random.key(seed), 12)
    acts = centred(arg_keys[0], (TOKENS, D), 1.0, 6.0, ((0, 128),))
    grad_keys = centred(arg_keys[1], (TOKENS, KV), (TOKENS // 4) ** -0.5, 0.03125, ((0, 128),))
    grad_values = centred(arg_keys[2], (TOKENS, KV), (TOKENS // 4) ** -0.5, 0.03125, ((0, 128),))
    grad_logits = centred(arg_keys[3], (EXPERTS, TOKENS), (TOKENS // 4) ** -0.5, 0.03125, ((1, 128),))
    order = jax.random.permutation(arg_keys[4], BLOCKS).astype(jnp.int32)
    bucket_param = centred(arg_keys[5], (BUCKETS, BUCKET_ROWS, KV), 1.0, 6.0, ((1, 16),), jnp.float32)
    bucket_m = centred(arg_keys[6], (BUCKETS, BUCKET_ROWS, KV), 1.0, 6.0, ((1, 16),), jnp.float32)
    bucket_v = jnp.clip(jnp.exp(math.log(4.0) - 2.7725887 * jax.random.uniform(arg_keys[7], (BUCKETS, BUCKET_ROWS, KV), jnp.float32) ** levels(arg_keys[7], (BUCKETS, BUCKET_ROWS, KV), ((1, 16),), -0.2, 0.2)), 0.25, 4.0)
    router_param = centred(arg_keys[8], (ROUTER_ROWS, KV), 1.0, 6.0, ((0, 16),), jnp.float32)
    router_m = centred(arg_keys[9], (ROUTER_ROWS, KV), 1.0, 6.0, ((0, 16),), jnp.float32)
    router_v = jnp.clip(jnp.exp(math.log(4.0) - 2.7725887 * jax.random.uniform(arg_keys[10], (ROUTER_ROWS, KV), jnp.float32) ** levels(arg_keys[10], (ROUTER_ROWS, KV), ((0, 16),), -0.2, 0.2)), 0.25, 4.0)
    return {"acts": acts, "grad_keys": grad_keys, "grad_values": grad_values, "grad_logits": grad_logits, "order": order, "bucket_param": bucket_param, "bucket_m": bucket_m, "bucket_v": bucket_v, "router_param": router_param, "router_m": router_m, "router_v": router_v}


beta_first = 0.9
beta_second = 0.95
step_rate = 0.05
decay_rate = 0.1
epsilon = 1e-08
correct_first = 1.0 - 0.9 ** 10
correct_second = 1.0 - 0.95 ** 10

def contract(left, right):
    return lax.dot_general(left, right, (((0,), (0,)), ((), ())), preferred_element_type=jnp.float32)

def adamw(grad, param, moment, second):
    moment_new = beta_first * moment + (1.0 - beta_first) * grad
    second_new = beta_second * second + (1.0 - beta_second) * grad * grad
    ratio = moment_new / correct_first / (jnp.sqrt(second_new / correct_second) + epsilon)
    param_new = param - step_rate * (ratio + decay_rate * param)
    return (param_new, moment_new, second_new)

def reference(acts, grad_keys, grad_values, grad_logits, order, bucket_param, bucket_m, bucket_v, router_param, router_m, router_v):
    weight_rows = jnp.concatenate([contract(acts, grad_keys), contract(acts, grad_values)], axis=0)
    blocks = weight_rows.reshape(BLOCKS, BLOCK_ROWS, KV)
    packed = jnp.take(blocks, order.astype(jnp.int32), axis=0).reshape(BUCKETS, BUCKET_ROWS, KV)
    router_grad = jnp.dot(grad_logits, acts, preferred_element_type=jnp.float32).reshape(ROUTER_ROWS, KV)
    new_param, new_moment, new_second = adamw(packed, bucket_param, bucket_m, bucket_v)
    router_new_param, router_new_moment, router_new_second = adamw(router_grad, router_param, router_m, router_v)
    return (new_param, new_moment, new_second, router_new_param, router_new_moment, router_new_second)
```

```python
import jax
import jax.numpy as jnp
from jax import lax
from jax.experimental import pallas as pl
from jax.experimental.pallas import tpu as pltpu
from jax.sharding import PartitionSpec as P

BUCKETS = 4
BLOCK_ROWS = 256
STEPS = 8
HALF = 512

beta_first = 0.9
beta_second = 0.95
step_rate = 0.05
decay_rate = 0.1
epsilon = 1e-08
correct_first = 1.0 - 0.9**10
correct_second = 1.0 - 0.95**10

MESH = pl.DeviceIdType.MESH
F32 = jnp.float32

DIMS = (("x", "y", "z"), ("y", "z", "x"), ("z", "x", "y"))
WIDTH = ((256, 128, 128), (128, 256, 128))
OFFSET = ((0, 256, 384), (256, 0, 384))


def adamw(grad, param, moment, second):
    moment_new = beta_first * moment + (1.0 - beta_first) * grad
    second_new = beta_second * second + (1.0 - beta_second) * grad * grad
    ratio = moment_new / correct_first / (jnp.sqrt(second_new / correct_second) + epsilon)
    param_new = param - step_rate * (ratio + decay_rate * param)
    return (param_new, moment_new, second_new)


def scratch():
    tree = {
        "acts": pltpu.VMEM((16, 1024, BLOCK_ROWS), jnp.bfloat16),
        "grads": pltpu.VMEM((2, 1024, 1024), jnp.bfloat16),
        "turned": pltpu.VMEM((BLOCK_ROWS, 1024), jnp.bfloat16),
        "out": pltpu.VMEM((BUCKETS, 2, 2, 4, 16, HALF), F32),
        "rt": pltpu.VMEM((2, 4, 2, 1, 2048), F32),
        "rx": pltpu.VMEM((4, 2, 1, 2048), F32),
        "rxx": pltpu.VMEM((3, 2, 1, 2048), F32),
        "rxy": pltpu.VMEM((4, 1, 2048), F32),
        "rxz": pltpu.VMEM((4, 1, 2048), F32),
        "ry": pltpu.VMEM((2, 1, 2048), F32),
        "load_sem": pltpu.SemaphoreType.DMA((18,)),
        "x_send": pltpu.SemaphoreType.DMA((STEPS, 3)),
        "x_recv": pltpu.SemaphoreType.DMA((STEPS, 3)),
        "p1_send": pltpu.SemaphoreType.DMA((STEPS, 3, 6)),
        "p1_recv": pltpu.SemaphoreType.DMA((STEPS, 3, 6)),
        "p2_send": pltpu.SemaphoreType.DMA((STEPS, 3, 6)),
        "p2_recv": pltpu.SemaphoreType.DMA((STEPS, 3, 6)),
        "p3_send": pltpu.SemaphoreType.DMA((STEPS, 3, 3)),
        "p3_recv": pltpu.SemaphoreType.DMA((STEPS, 3, 3)),
        "ag_send": pltpu.SemaphoreType.DMA((STEPS, 5)),
        "ag_recv": pltpu.SemaphoreType.DMA((STEPS, 5)),
        "r_send": pltpu.SemaphoreType.DMA((10,)),
        "r_recv": pltpu.SemaphoreType.DMA((10,)),
        "out_sem": pltpu.SemaphoreType.DMA((STEPS,)),
    }
    for parity in range(2):
        for colour in range(3):
            w = WIDTH[parity][colour]
            tail = f"{parity}{colour}"
            tree["px" + tail] = pltpu.VMEM((2, 4, 4, 4, 16, w), F32)
            tree["xr" + tail] = pltpu.VMEM((2, 4, 4, 4, 16, w), F32)
            tree["ra" + tail] = pltpu.VMEM((BUCKETS, 6, 2, 4, 16, w), F32)
            tree["q" + tail] = pltpu.VMEM((BUCKETS, 4, 4, 16, w), F32)
            tree["rb" + tail] = pltpu.VMEM((BUCKETS, 6, 2, 16, w), F32)
            tree["rc" + tail] = pltpu.VMEM((BUCKETS, 3, 16, w), F32)
    return tree


def kernel(names, order, logits, acts_hbm, keys_hbm, values_hbm, out_hbm, router_out, *refs):
    ref = dict(zip(names, refs))
    rep = lax.axis_index("rep")
    inst = lax.axis_index("inst")
    yl, z = rep // 4, rep % 4
    yh, x, core = inst // 8, (inst // 2) % 4, inst % 2
    place = {"x": x, "y": yh * 2 + yl, "z": z, "c": core}

    def device(**change):
        at = {**place, **change}
        y = at["y"]
        return {"rep": (y % 2) * 4 + at["z"], "inst": ((y // 2) * 4 + at["x"]) * 2 + at["c"]}

    def along(dim, delta):
        return device(**{dim: (place[dim] + delta) % 4})

    sibling = device(c=1 - core)
    partner = device(y=yh * 2 + (1 - yl))

    def send(src, dst, send_sem, recv_sem, to):
        copy = pltpu.make_async_remote_copy(
            src_ref=src, dst_ref=dst, send_sem=send_sem, recv_sem=recv_sem, device_id=to, device_id_type=MESH
        )
        copy.start()

    def wait_recv(dst, sem):
        pltpu.make_async_copy(dst, dst, sem).wait()

    wait_send = wait_recv

    loads = []
    for i in range(16):
        loads.append(
            pltpu.make_async_copy(
                acts_hbm.at[:, i * BLOCK_ROWS : (i + 1) * BLOCK_ROWS], ref["acts"].at[i], ref["load_sem"].at[i]
            )
        )
    loads.append(pltpu.make_async_copy(keys_hbm, ref["grads"].at[0], ref["load_sem"].at[16]))
    loads.append(pltpu.make_async_copy(values_hbm, ref["grads"].at[1], ref["load_sem"].at[17]))
    for load in loads:
        load.start()

    barrier = pltpu.get_barrier_semaphore()
    peers = [sibling] + [along(d, delta) for d in "xyz" for delta in (1, 2, 3)]
    for peer in peers:
        pl.semaphore_signal(barrier, inc=1, device_id=peer, device_id_type=MESH)

    for i in range(16):
        loads[i].wait()
        term = jnp.dot(logits[...], ref["acts"][i], preferred_element_type=F32)
        for e in range(8):
            ref["rt"][i // 8, e % 4, e // 4, :, pl.ds((i % 8) * 256, 256)] = term[e : e + 1, :]
    loads[16].wait()
    loads[17].wait()

    def matmul(step, first, last):
        bucket, parity = step // 2, step % 2

        def body(j, carry):
            slot_y, slot_x = j // 4, j % 4
            block = order[bucket * 8 + j]
            ref["turned"][...] = ref["acts"][block % 16].T
            for n in range(2):
                lo = n * 256
                piece = jnp.dot(
                    ref["turned"][...],
                    ref["grads"][block // 16, :, parity * HALF + lo : parity * HALF + lo + 256],
                    preferred_element_type=F32,
                )
                for colour in range(3):
                    w, off = WIDTH[parity][colour], OFFSET[parity][colour]
                    if not lo <= off < lo + 256:
                        continue
                    px = ref[f"px{parity}{colour}"]
                    part = piece[:, off - lo : off - lo + w]
                    for h in range(2):
                        for l in range(2):
                            rows = part[h * 128 + l * 64 : h * 128 + l * 64 + 64].reshape(4, 16, w)
                            y = slot_y * 2 + l
                            if colour == 0:
                                px[h, slot_x, y] = rows
                            elif colour == 1:
                                for k in range(4):
                                    px[h, y, k, slot_x] = rows[k]
                            else:
                                for k in range(4):
                                    px[h, k, slot_x, y] = rows[k]
            return carry

        lax.fori_loop(first, last, body, 0)

    def exchange(step):
        b, par = step // 2, step % 2
        for q in range(3):
            send(
                ref[f"px{par}{q}"].at[1 - core],
                ref[f"xr{par}{q}"].at[b % 2],
                ref["x_send"].at[step, q],
                ref["x_recv"].at[step, q],
                sibling,
            )

    def add_sibling(step):
        b, par = step // 2, step % 2
        for q in range(3):
            px, xr = ref[f"px{par}{q}"], ref[f"xr{par}{q}"]
            wait_recv(xr.at[b % 2], ref["x_recv"].at[step, q])

            def body(d, carry):
                px[core, d] = px[core, d] + xr[b % 2, d]
                return carry

            lax.fori_loop(0, 4, body, 0)

    def views(step, q, phase):
        b, par = step // 2, step % 2
        if phase == 1:
            px, recv = ref[f"px{par}{q}"], ref[f"ra{par}{q}"]
            return px, (lambda d, h: (core, d, pl.ds(2 * h, 2))), recv, b
        src, recv = ref[f"q{par}{q}"], ref[f"rb{par}{q}"]
        return src, (lambda d, h: (b, d, pl.ds(2 * h, 2))), recv, b

    def ring_send(step, q, phase, m, where, delta):
        src, at, recv, b = views(step, q, phase)
        dim = DIMS[q][phase - 1]
        d, h = where
        send(
            src.at[at((place[dim] + d) % 4, h)],
            recv.at[b, m],
            ref[f"p{phase}_send"].at[step, q, m],
            ref[f"p{phase}_recv"].at[step, q, m],
            along(dim, delta),
        )

    def ring_start(step, phase):
        for q in range(3):
            ring_send(step, q, phase, 0, (2, 0), 1)
            ring_send(step, q, phase, 1, (2, 1), 3)
            ring_send(step, q, phase, 2, (1, 1), 1)
            ring_send(step, q, phase, 3, (3, 0), 3)

    def ring_relay(step, phase):
        for q in range(3):
            src, at, recv, b = views(step, q, phase)
            here = place[DIMS[q][phase - 1]]
            for m, d, h in ((0, 1, 0), (1, 3, 1)):
                wait_recv(recv.at[b, m], ref[f"p{phase}_recv"].at[step, q, m])
                spot = at((here + d) % 4, h)
                src[spot] = src[spot] + recv[b, m]
                ring_send(step, q, phase, 4 + m, (d, h), d)

    def ring_end(step, phase):
        b, par = step // 2, step % 2
        for q in range(3):
            src, at, recv, _ = views(step, q, phase)
            here = place[DIMS[q][phase - 1]]
            for h, arrived in ((0, (3, 4)), (1, (2, 5))):
                for m in arrived:
                    wait_recv(recv.at[b, m], ref[f"p{phase}_recv"].at[step, q, m])
                spot = at(here, h)
                total = src[spot] + recv[b, arrived[0]] + recv[b, arrived[1]]
                if phase == 1:
                    ref[f"q{par}{q}"][b, pl.ds(2 * h, 2)] = total
                else:
                    src[spot] = total

    def ring_sent(step, phase):
        for q in range(3):
            recv = views(step, q, phase)[2]
            for m in range(6):
                wait_send(recv.at[step // 2, m], ref[f"p{phase}_send"].at[step, q, m])

    def exchange_sent(step):
        for q in range(3):
            wait_send(ref[f"xr{step % 2}{q}"].at[step // 2 % 2], ref["x_send"].at[step, q])

    def last_start(step):
        b, par = step // 2, step % 2
        for q in range(3):
            second, third = DIMS[q][1:]
            for m in range(3):
                delta = (1, 3, 2)[m]
                send(
                    ref[f"q{par}{q}"].at[b, place[second], (place[third] + delta) % 4],
                    ref[f"rc{par}{q}"].at[b, m],
                    ref["p3_send"].at[step, q, m],
                    ref["p3_recv"].at[step, q, m],
                    along(third, delta),
                )

    def last_end(step):
        b, par = step // 2, step % 2
        for q in range(3):
            second, third = DIMS[q][1:]
            rc = ref[f"rc{par}{q}"]
            for m in range(3):
                wait_recv(rc.at[b, m], ref["p3_recv"].at[step, q, m])
            total = ref[f"q{par}{q}"][b, place[second], place[third]] + rc[b, 0] + rc[b, 1] + rc[b, 2]
            ref["out"][b, par, yl, z, :, pl.ds(OFFSET[par][q], WIDTH[par][q])] = total

    def last_sent(step):
        for q in range(3):
            for m in range(3):
                wait_send(ref[f"rc{step % 2}{q}"].at[step // 2, m], ref["p3_send"].at[step, q, m])

    def gather_send(step, n, spot, to):
        out = ref["out"].at[(step // 2, step % 2) + spot]
        send(out, out, ref["ag_send"].at[step, n], ref["ag_recv"].at[step, n], to)

    def gather_wait(step, n, spot, which="ag_recv"):
        wait_recv(ref["out"].at[(step // 2, step % 2) + spot], ref[which].at[step, n])

    both = pl.ds(0, 2)

    def gather_partner(step):
        gather_send(step, 0, (yl, z), partner)

    def gather_start(step):
        gather_wait(step, 0, (1 - yl, z))
        gather_send(step, 1, (both, z), along("z", 1))
        gather_send(step, 2, (both, z), along("z", 3))

    def gather_relay(step):
        gather_wait(step, 1, (both, (z + 3) % 4))
        gather_send(step, 3, (0, (z + 3) % 4), along("z", 1))
        gather_wait(step, 2, (both, (z + 1) % 4))
        gather_send(step, 4, (1, (z + 1) % 4), along("z", 3))

    def gather_end(step):
        gather_wait(step, 3, (0, (z + 2) % 4))
        gather_wait(step, 4, (1, (z + 2) % 4))
        b, par = step // 2, step % 2
        pltpu.make_async_copy(
            ref["out"].at[b, par], out_hbm.at[b, :, :, :, pl.ds(par * HALF, HALF)], ref["out_sem"].at[step]
        ).start()

    def gather_sent(step):
        for n, spot in enumerate(((yl, z), (both, z), (both, z), (0, z), (1, z))):
            gather_wait(step, n, spot, "ag_send")
        b, par = step // 2, step % 2
        pltpu.make_async_copy(
            ref["out"].at[b, par], out_hbm.at[b, :, :, :, pl.ds(par * HALF, HALF)], ref["out_sem"].at[step]
        ).wait()

    def router_send(n, src, dst, to):
        send(src, dst, ref["r_send"].at[n], ref["r_recv"].at[n], to)

    def router_wait(n, dst):
        wait_recv(dst, ref["r_recv"].at[n])

    def router_0():
        router_send(0, ref["rt"].at[1 - core], ref["rx"], sibling)

    def router_1():
        router_wait(0, ref["rx"])
        ref["rt"][core] = ref["rt"][core] + ref["rx"][...]
        for m, delta in enumerate((1, 2, 3)):
            router_send(1 + m, ref["rt"].at[core, (x + delta) % 4], ref["rxx"].at[m], along("x", delta))

    def router_2():
        for m in range(3):
            router_wait(1 + m, ref["rxx"].at[m])
        ref["ry"][...] = ref["rt"][core, x] + ref["rxx"][0] + ref["rxx"][1] + ref["rxx"][2]
        here = place["y"]
        ref["rxy"][here] = ref["ry"][yh]
        for m, delta in enumerate((1, 2, 3)):
            to = (here + delta) % 4
            router_send(4 + m, ref["ry"].at[to // 2], ref["rxy"].at[here], along("y", delta))

    def router_3():
        here = place["y"]
        for m, delta in enumerate((1, 2, 3)):
            router_wait(4 + m, ref["rxy"].at[(here - delta) % 4])
        total = ref["rxy"][0] + ref["rxy"][1] + ref["rxy"][2] + ref["rxy"][3]
        ref["rxz"][z] = total
        for m, delta in enumerate((1, 2, 3)):
            router_send(7 + m, ref["rxz"].at[z], ref["rxz"].at[z], along("z", delta))

    def router_4():
        for m, delta in enumerate((1, 2, 3)):
            router_wait(7 + m, ref["rxz"].at[(z - delta) % 4])
        router_out[...] = ref["rxz"][0] + ref["rxz"][1] + ref["rxz"][2] + ref["rxz"][3]

    def router_sent():
        wait_send(ref["rx"], ref["r_send"].at[0])
        for m in range(3):
            wait_send(ref["rxx"].at[m], ref["r_send"].at[1 + m])
            wait_send(ref["rxy"].at[m], ref["r_send"].at[4 + m])
            wait_send(ref["rxz"].at[m], ref["r_send"].at[7 + m])

    router_stages = {0: router_0, 1: router_1, 2: router_2, 3: router_3, 4: router_4}

    matmul(0, 0, 8)
    pl.semaphore_wait(barrier, len(peers))
    exchange(0)
    for i in range(STEPS + 4):
        def live(step):
            return 0 <= step < STEPS

        if live(i):
            add_sibling(i)
            ring_start(i, 1)
        if live(i - 1):
            ring_end(i - 1, 1)
            ring_start(i - 1, 2)
        if live(i - 2):
            ring_end(i - 2, 2)
            last_start(i - 2)
        if live(i - 3):
            gather_start(i - 3)
        if live(i - 4):
            gather_end(i - 4)
        if i in router_stages:
            router_stages[i]()
        if live(i + 1):
            if live(i - 1):
                exchange_sent(i - 1)
                ring_sent(i - 1, 1)
            matmul(i + 1, 0, 8)
            exchange(i + 1)
        if live(i):
            ring_relay(i, 1)
        if live(i - 1):
            ring_relay(i - 1, 2)
        if live(i - 2):
            last_end(i - 2)
            gather_partner(i - 2)
        if live(i - 3):
            gather_relay(i - 3)
    for step in range(STEPS):
        if step >= STEPS - 2:
            exchange_sent(step)
            ring_sent(step, 1)
        ring_sent(step, 2)
        last_sent(step)
        gather_sent(step)
    router_sent()


def on_device(
    acts,
    grad_keys,
    grad_values,
    grad_logits,
    order,
    bucket_param,
    bucket_m,
    bucket_v,
    router_param,
    router_m,
    router_v,
):
    tree = scratch()
    names = tuple(tree)
    hbm = pl.BlockSpec(memory_space=pltpu.HBM)
    grad, router_grad = pl.pallas_call(
        lambda *refs: kernel(names, *refs),
        out_shape=(
            jax.ShapeDtypeStruct((BUCKETS, 2, 4, 16, 1024), F32),
            jax.ShapeDtypeStruct((1, 2048), F32),
        ),
        in_specs=[
            pl.BlockSpec(memory_space=pltpu.SMEM),
            pl.BlockSpec(memory_space=pltpu.VMEM),
            hbm,
            hbm,
            hbm,
        ],
        out_specs=(hbm, pl.BlockSpec(memory_space=pltpu.VMEM)),
        scratch_shapes=list(tree.values()),
        compiler_params=pltpu.CompilerParams(
            collective_id=0, has_side_effects=True, vmem_limit_bytes=58 * 1024 * 1024
        ),
        cost_estimate=pl.CostEstimate(flops=17_200_000_000, bytes_accessed=16_000_000, transcendentals=0),
        name="reduce",
    )(order, grad_logits, acts, grad_keys, grad_values)
    fresh = adamw(grad.reshape(bucket_param.shape), bucket_param, bucket_m, bucket_v)
    router_fresh = adamw(router_grad.reshape(router_param.shape), router_param, router_m, router_v)
    return fresh + router_fresh


def solution(mesh):
    state, router = P(None, "inst", None), P("inst", None)
    tokens = P(("rep", "inst"), None)
    return jax.shard_map(
        on_device,
        mesh=mesh,
        in_specs=(tokens, tokens, tokens, P(None, ("rep", "inst")), P(), state, state, state, router, router, router),
        out_specs=(state, state, state, router, router, router),
        check_vma=False,
    )
```

```python
import jax
import jax.numpy as jnp
from jax import lax
from jax.experimental import pallas as pl
from jax.experimental.pallas import tpu as pltpu
from jax.sharding import PartitionSpec as P

BUCKETS = 4
BLOCK_ROWS = 256
STEPS = 8
HALF = 512

beta_first = 0.9
beta_second = 0.95
step_rate = 0.05
decay_rate = 0.1
epsilon = 1e-08
correct_first = 1.0 - 0.9**10
correct_second = 1.0 - 0.95**10

VMEM_LIMIT = 56 * 1024 * 1024
MESH = pl.DeviceIdType.MESH
F32 = jnp.float32

DIMS = (("x", "y", "z"), ("y", "z", "x"), ("z", "x", "y"))
PARTS = (((0, 0, 16, 0), (3, 0, 8, 16)), ((1, 0, 16, 0), (3, 8, 8, 16)), ((2, 0, 16, 0),))
ROWS = (24, 24, 16)
W = 128
OWN = 4
SENT = 2


def adamw(grad, param, moment, second):
    moment_new = beta_first * moment + (1.0 - beta_first) * grad
    second_new = beta_second * second + (1.0 - beta_second) * grad * grad
    ratio = moment_new / correct_first / (jnp.sqrt(second_new / correct_second) + epsilon)
    param_new = param - step_rate * (ratio + decay_rate * param)
    return (param_new, moment_new, second_new)


def scratch():
    tree = {
        "acts": pltpu.VMEM((16, 1024, BLOCK_ROWS), jnp.bfloat16),
        "grads": pltpu.VMEM((2, 1024, 1024), jnp.bfloat16),
        "turned": pltpu.VMEM((BLOCK_ROWS, 1024), jnp.bfloat16),
        "out": pltpu.VMEM((BUCKETS, 2, 2, 4, 16, HALF), F32),
        "rt": pltpu.VMEM((2, 4, 2, 1, 2048), F32),
        "rx": pltpu.VMEM((4, 2, 1, 2048), F32),
        "rxx": pltpu.VMEM((3, 2, 1, 2048), F32),
        "rxy": pltpu.VMEM((4, 1, 2048), F32),
        "rxz": pltpu.VMEM((4, 1, 2048), F32),
        "ry": pltpu.VMEM((2, 1, 2048), F32),
        "load_sem": pltpu.SemaphoreType.DMA((18,)),
        "state_sem": pltpu.SemaphoreType.DMA((3,)),
        "x_send": pltpu.SemaphoreType.DMA((STEPS, 3)),
        "x_recv": pltpu.SemaphoreType.DMA((STEPS, 3)),
        "p1_send": pltpu.SemaphoreType.DMA((STEPS, 3, 6)),
        "p1_recv": pltpu.SemaphoreType.DMA((STEPS, 3, 6)),
        "p2_send": pltpu.SemaphoreType.DMA((STEPS, 3, 6)),
        "p2_recv": pltpu.SemaphoreType.DMA((STEPS, 3, 6)),
        "p3_send": pltpu.SemaphoreType.DMA((STEPS, 3, 3)),
        "p3_recv": pltpu.SemaphoreType.DMA((STEPS, 3, 3)),
        "ag_send": pltpu.SemaphoreType.DMA((STEPS, 5)),
        "ag_recv": pltpu.SemaphoreType.DMA((STEPS, 5)),
        "r_send": pltpu.SemaphoreType.DMA((10,)),
        "r_recv": pltpu.SemaphoreType.DMA((10,)),
    }
    for q in range(3):
        r = ROWS[q]
        tree[f"own{q}"] = pltpu.VMEM((OWN, 4, 4, 4, r, W), F32)
        tree[f"sent{q}"] = pltpu.VMEM((SENT, 4, 4, 4, r, W), F32)
        tree[f"xr{q}"] = pltpu.VMEM((4, 4, 4, 4, r, W), F32)
        tree[f"ra{q}"] = pltpu.VMEM((4, 6, 2, 4, r, W), F32)
        tree[f"q{q}"] = pltpu.VMEM((STEPS, 4, 4, r, W), F32)
        tree[f"rb{q}"] = pltpu.VMEM((STEPS, 6, 2, r, W), F32)
        tree[f"rc{q}"] = pltpu.VMEM((STEPS, 3, r, W), F32)
    return tree


def kernel(names, order, logits, acts_hbm, keys_hbm, values_hbm, *refs):
    state_hbm, router_state = refs[0:3], refs[3:6]
    state, router_new = refs[6:9], refs[9:12]
    refs = refs[12:]
    ref = dict(zip(names, refs))
    rep = lax.axis_index("rep")
    inst = lax.axis_index("inst")
    yl, z = rep // 4, rep % 4
    yh, x, core = inst // 8, (inst // 2) % 4, inst % 2
    place = {"x": x, "y": yh * 2 + yl, "z": z, "c": core}

    def device(**change):
        at = {**place, **change}
        y = at["y"]
        return {"rep": (y % 2) * 4 + at["z"], "inst": ((y // 2) * 4 + at["x"]) * 2 + at["c"]}

    def along(dim, delta):
        return device(**{dim: (place[dim] + delta) % 4})

    sibling = device(c=1 - core)
    partner = device(y=yh * 2 + (1 - yl))

    def send(src, dst, send_sem, recv_sem, to):
        copy = pltpu.make_async_remote_copy(
            src_ref=src, dst_ref=dst, send_sem=send_sem, recv_sem=recv_sem, device_id=to, device_id_type=MESH
        )
        copy.start()

    def wait_recv(dst, sem):
        pltpu.make_async_copy(dst, dst, sem).wait()

    wait_send = wait_recv

    loads = [
        pltpu.make_async_copy(keys_hbm, ref["grads"].at[0], ref["load_sem"].at[16]),
        pltpu.make_async_copy(values_hbm, ref["grads"].at[1], ref["load_sem"].at[17]),
    ]
    for i in range(16):
        loads.append(
            pltpu.make_async_copy(
                acts_hbm.at[:, i * BLOCK_ROWS : (i + 1) * BLOCK_ROWS], ref["acts"].at[i], ref["load_sem"].at[i]
            )
        )
    for load in loads:
        load.start()
    state_loads = [pltpu.make_async_copy(state_hbm[n], state[n], ref["state_sem"].at[n]) for n in range(3)]

    barrier = pltpu.get_barrier_semaphore()
    peers = [sibling] + [along(d, delta) for d in "xyz" for delta in (1, 2, 3)]
    for peer in peers:
        pl.semaphore_signal(barrier, inc=1, device_id=peer, device_id_type=MESH)

    def router_term():
        for i in range(16):
            term = jnp.dot(logits[...], ref["acts"][i], preferred_element_type=F32)
            for e in range(8):
                ref["rt"][i // 8, e % 4, e // 4, :, pl.ds((i % 8) * 256, 256)] = term[e : e + 1, :]

    def spots(q, slot_y, slot_x):
        if q == 0:
            return (slot_x, pl.ds(slot_y * 2, 2))
        if q == 1:
            return (pl.ds(slot_y * 2, 2), pl.ds(0, 4), slot_x)
        return (pl.ds(0, 4), slot_x, pl.ds(slot_y * 2, 2))

    def exchange(step, j):
        for q in range(3):
            spot = spots(q, j // 4, j % 4)
            send(
                ref[f"sent{q}"].at[(step % SENT,) + spot],
                ref[f"xr{q}"].at[(step % 4,) + spot],
                ref["x_send"].at[step, q],
                ref["x_recv"].at[step, q],
                sibling,
            )

    def matmul(step, first, last):
        bucket, par = step // 2, step % 2

        def body(j, carry):
            slot_y, slot_x = j // 4, j % 4
            block = order[bucket * 8 + j]
            for h, side in enumerate((core, 1 - core)):
                columns = ref["acts"][block % 16, :, pl.ds(pl.multiple_of(side * 128, 128), 128)]
                ref["turned"][h * 128 : (h + 1) * 128] = columns.T
            for n in range(2):
                lo = n * 256
                piece = jnp.dot(
                    ref["turned"][...],
                    ref["grads"][block // 16, :, par * HALF + lo : par * HALF + lo + 256],
                    preferred_element_type=F32,
                )
                for h in range(2):
                    dst = "sent" if h else "own"
                    slot = step % (SENT if h else OWN)
                    for q in range(3):
                        for chunk, top, count, row in PARTS[q]:
                            if chunk // 2 != n:
                                continue
                            left = chunk % 2 * W
                            for l in range(2):
                                y = slot_y * 2 + l
                                for k in range(4):
                                    start = h * 128 + l * 64 + k * 16 + top
                                    value = piece[start : start + count, left : left + W]
                                    at = ((slot_x, y, k), (y, k, slot_x), (k, slot_x, y))[q]
                                    ref[f"{dst}{q}"][(slot,) + at + (pl.ds(row, count),)] = value

            @pl.when(j > first)
            def _():
                exchange(step, j - 1)

            return carry

        lax.fori_loop(first, last, body, 0)
        exchange(step, last - 1)

    def add_sibling(step):
        for q in range(3):
            own, xr = ref[f"own{q}"], ref[f"xr{q}"]
            wait_recv(xr.at[step % 4], ref["x_recv"].at[step, q])

            def body(d, carry):
                own[step % OWN, d] = own[step % OWN, d] + xr[step % 4, d]
                return carry

            lax.fori_loop(0, 4, body, 0)

    def views(step, q, phase):
        slot = step % OWN if phase == 1 else step
        src, recv = (ref[f"own{q}"], ref[f"ra{q}"]) if phase == 1 else (ref[f"q{q}"], ref[f"rb{q}"])
        return src, (lambda d, h: (slot, d, pl.ds(2 * h, 2))), recv, (step % 4 if phase == 1 else step)

    def ring_send(step, q, phase, m, where, delta):
        src, at, recv, b = views(step, q, phase)
        dim = DIMS[q][phase - 1]
        d, h = where
        send(
            src.at[at((place[dim] + d) % 4, h)],
            recv.at[b, m],
            ref[f"p{phase}_send"].at[step, q, m],
            ref[f"p{phase}_recv"].at[step, q, m],
            along(dim, delta),
        )

    def ring_start(step, phase):
        for q in range(3):
            ring_send(step, q, phase, 0, (2, 0), 1)
            ring_send(step, q, phase, 1, (2, 1), 3)
            ring_send(step, q, phase, 2, (1, 1), 1)
            ring_send(step, q, phase, 3, (3, 0), 3)

    def ring_relay(step, phase):
        for q in range(3):
            src, at, recv, b = views(step, q, phase)
            here = place[DIMS[q][phase - 1]]
            for m, d, h in ((0, 1, 0), (1, 3, 1)):
                wait_recv(recv.at[b, m], ref[f"p{phase}_recv"].at[step, q, m])
                spot = at((here + d) % 4, h)
                src[spot] = src[spot] + recv[b, m]
                ring_send(step, q, phase, 4 + m, (d, h), d)

    def ring_end(step, phase):
        for q in range(3):
            src, at, recv, b = views(step, q, phase)
            here = place[DIMS[q][phase - 1]]
            for h, arrived in ((0, (3, 4)), (1, (2, 5))):
                for m in arrived:
                    wait_recv(recv.at[b, m], ref[f"p{phase}_recv"].at[step, q, m])
                spot = at(here, h)
                total = src[spot] + recv[b, arrived[0]] + recv[b, arrived[1]]
                if phase == 1:
                    ref[f"q{q}"][step, pl.ds(2 * h, 2)] = total
                else:
                    src[spot] = total

    def ring_sent(step, phase):
        for q in range(3):
            _, _, recv, b = views(step, q, phase)
            for m in range(6):
                wait_send(recv.at[b, m], ref[f"p{phase}_send"].at[step, q, m])

    def exchange_sent(step):
        for q in range(3):
            wait_send(ref[f"xr{q}"].at[step % 4], ref["x_send"].at[step, q])

    def last_start(step):
        for q in range(3):
            second, third = DIMS[q][1:]
            for m in range(3):
                delta = (1, 3, 2)[m]
                send(
                    ref[f"q{q}"].at[step, place[second], (place[third] + delta) % 4],
                    ref[f"rc{q}"].at[step, m],
                    ref["p3_send"].at[step, q, m],
                    ref["p3_recv"].at[step, q, m],
                    along(third, delta),
                )

    def last_end(step):
        b, par = step // 2, step % 2
        for q in range(3):
            second, third = DIMS[q][1:]
            rc = ref[f"rc{q}"]
            for m in range(3):
                wait_recv(rc.at[step, m], ref["p3_recv"].at[step, q, m])
            total = ref[f"q{q}"][step, place[second], place[third]] + rc[step, 0] + rc[step, 1] + rc[step, 2]
            for chunk, top, count, row in PARTS[q]:
                ref["out"][b, par, yl, z, pl.ds(top, count), pl.ds(chunk * W, W)] = total[row : row + count]

    def last_sent(step):
        for q in range(3):
            for m in range(3):
                wait_send(ref[f"rc{q}"].at[step, m], ref["p3_send"].at[step, q, m])

    def gather_send(step, n, spot, to):
        out = ref["out"].at[(step // 2, step % 2) + spot]
        send(out, out, ref["ag_send"].at[step, n], ref["ag_recv"].at[step, n], to)

    def gather_wait(step, n, spot, which="ag_recv"):
        wait_recv(ref["out"].at[(step // 2, step % 2) + spot], ref[which].at[step, n])

    both = pl.ds(0, 2)

    def gather_partner(step):
        gather_send(step, 0, (yl, z), partner)

    def gather_start(step):
        gather_wait(step, 0, (1 - yl, z))
        gather_send(step, 1, (both, z), along("z", 1))
        gather_send(step, 2, (both, z), along("z", 3))

    def gather_relay(step):
        gather_wait(step, 1, (both, (z + 3) % 4))
        gather_send(step, 3, (0, (z + 3) % 4), along("z", 1))
        gather_wait(step, 2, (both, (z + 1) % 4))
        gather_send(step, 4, (1, (z + 1) % 4), along("z", 3))

    def gather_end(step):
        gather_wait(step, 3, (0, (z + 2) % 4))
        gather_wait(step, 4, (1, (z + 2) % 4))
        b, par = step // 2, step % 2
        columns = pl.ds(par * HALF, HALF)

        def body(i, carry):
            rows = pl.ds(pl.multiple_of(i * 16, 16), 16)
            grad = ref["out"][b, par, i // 4, i % 4]
            fresh = adamw(grad, *(part[b, rows, columns] for part in state))
            for part, value in zip(state, fresh):
                part[b, rows, columns] = value
            return carry

        lax.fori_loop(0, 8, body, 0)

    def gather_sent(step):
        for n, spot in enumerate(((yl, z), (both, z), (both, z), (0, z), (1, z))):
            gather_wait(step, n, spot, "ag_send")

    def state_start():
        for load in state_loads:
            load.start()

    def state_end():
        for load in state_loads:
            load.wait()

    def router_send(n, src, dst, to):
        send(src, dst, ref["r_send"].at[n], ref["r_recv"].at[n], to)

    def router_wait(n, dst):
        wait_recv(dst, ref["r_recv"].at[n])

    def router_0():
        router_send(0, ref["rt"].at[1 - core], ref["rx"], sibling)

    def router_1():
        router_wait(0, ref["rx"])
        ref["rt"][core] = ref["rt"][core] + ref["rx"][...]
        for m, delta in enumerate((1, 2, 3)):
            router_send(1 + m, ref["rt"].at[core, (x + delta) % 4], ref["rxx"].at[m], along("x", delta))

    def router_2():
        for m in range(3):
            router_wait(1 + m, ref["rxx"].at[m])
        ref["ry"][...] = ref["rt"][core, x] + ref["rxx"][0] + ref["rxx"][1] + ref["rxx"][2]
        here = place["y"]
        ref["rxy"][here] = ref["ry"][yh]
        for m, delta in enumerate((1, 2, 3)):
            to = (here + delta) % 4
            router_send(4 + m, ref["ry"].at[to // 2], ref["rxy"].at[here], along("y", delta))

    def router_3():
        here = place["y"]
        for m, delta in enumerate((1, 2, 3)):
            router_wait(4 + m, ref["rxy"].at[(here - delta) % 4])
        total = ref["rxy"][0] + ref["rxy"][1] + ref["rxy"][2] + ref["rxy"][3]
        ref["rxz"][z] = total
        for m, delta in enumerate((1, 2, 3)):
            router_send(7 + m, ref["rxz"].at[z], ref["rxz"].at[z], along("z", delta))

    def router_4():
        for m, delta in enumerate((1, 2, 3)):
            router_wait(7 + m, ref["rxz"].at[(z - delta) % 4])
        total = ref["rxz"][0] + ref["rxz"][1] + ref["rxz"][2] + ref["rxz"][3]
        for row in range(2):
            at = pl.ds(row, 1)
            fresh = adamw(total[:, row * 1024 : (row + 1) * 1024], *(part[at] for part in router_state))
            for part, value in zip(router_new, fresh):
                part[at] = value

    def router_sent():
        wait_send(ref["rx"], ref["r_send"].at[0])
        for m in range(3):
            wait_send(ref["rxx"].at[m], ref["r_send"].at[1 + m])
            wait_send(ref["rxy"].at[m], ref["r_send"].at[4 + m])
            wait_send(ref["rxz"].at[m], ref["r_send"].at[7 + m])

    router_stages = {0: router_0, 1: router_1, 2: router_2, 3: router_3, 4: router_4}

    def run(stage, *args):
        with jax.named_scope(f"{stage.__name__}#s={'_'.join(map(str, args))}"):
            stage(*args)

    def live(step):
        return 0 <= step < STEPS

    with jax.named_scope("loads"):
        for load in loads:
            load.wait()
    with jax.named_scope("barrier"):
        pl.semaphore_wait(barrier, len(peers))
    run(matmul, 0, 0, 8)
    run(router_term)
    state_start()
    run(router_0)
    run(add_sibling, 0)
    run(ring_start, 0, 1)
    run(matmul, 1, 0, 8)
    for i in range(STEPS + 4):
        if live(i + 2):
            if live(i):
                run(exchange_sent, i)
            if live(i - 2):
                run(ring_sent, i - 2, 1)
            run(matmul, i + 2, 0, 4)
        if live(i - 2):
            run(ring_end, i - 2, 2)
            run(last_start, i - 2)
        if live(i - 1):
            run(ring_end, i - 1, 1)
            run(ring_start, i - 1, 2)
        if live(i - 3):
            run(gather_start, i - 3)
        if live(i + 2):
            run(matmul, i + 2, 4, 8)
        if live(i):
            run(ring_relay, i, 1)
        if live(i + 1):
            run(add_sibling, i + 1)
            run(ring_start, i + 1, 1)
        if live(i - 1):
            run(ring_relay, i - 1, 2)
        if live(i - 2):
            run(last_end, i - 2)
            run(gather_partner, i - 2)
        if live(i - 3):
            run(gather_relay, i - 3)
        if i + 1 in router_stages:
            run(router_stages[i + 1])
        if live(i - 4):
            if i == 4:
                run(state_end)
            run(gather_end, i - 4)
    with jax.named_scope("ending"):
        for step in range(STEPS):
            if step >= STEPS - 2:
                exchange_sent(step)
            if step >= STEPS - 4:
                ring_sent(step, 1)
            ring_sent(step, 2)
            last_sent(step)
            gather_sent(step)
        router_sent()


def on_device(
    acts,
    grad_keys,
    grad_values,
    grad_logits,
    order,
    bucket_param,
    bucket_m,
    bucket_v,
    router_param,
    router_m,
    router_v,
):
    tree = scratch()
    names = tuple(tree)
    hbm, vmem = pl.BlockSpec(memory_space=pltpu.HBM), pl.BlockSpec(memory_space=pltpu.VMEM)
    return pl.pallas_call(
        lambda *refs: kernel(names, *refs),
        out_shape=tuple(
            pltpu.VMEM(part.shape, F32) for part in (bucket_param, bucket_m, bucket_v, router_param, router_m, router_v)
        ),
        in_specs=[pl.BlockSpec(memory_space=pltpu.SMEM), vmem] + [hbm] * 6 + [vmem] * 3,
        out_specs=(vmem,) * 6,
        scratch_shapes=list(tree.values()),
        compiler_params=pltpu.CompilerParams(
            collective_id=0, has_side_effects=True, vmem_limit_bytes=VMEM_LIMIT
        ),
        cost_estimate=pl.CostEstimate(flops=17_200_000_000, bytes_accessed=24_000_000, transcendentals=0),
        name="reduce",
    )(
        order,
        grad_logits,
        acts,
        grad_keys,
        grad_values,
        bucket_param,
        bucket_m,
        bucket_v,
        router_param,
        router_m,
        router_v,
    )


def solution(mesh):
    state, router = P(None, "inst", None), P("inst", None)
    tokens = P(("rep", "inst"), None)
    return jax.shard_map(
        on_device,
        mesh=mesh,
        in_specs=(tokens, tokens, tokens, P(None, ("rep", "inst")), P(), state, state, state, router, router, router),
        out_specs=(state, state, state, router, router, router),
        check_vma=False,
    )
```

```python
import jax
import jax.numpy as jnp
from jax import lax
from jax.experimental import pallas as pl
from jax.experimental.pallas import tpu as pltpu
from jax.sharding import PartitionSpec as P

BUCKETS = 4
BLOCK_ROWS = 256
STEPS = 8
HALF = 512

beta_first = 0.9
beta_second = 0.95
step_rate = 0.05
decay_rate = 0.1
epsilon = 1e-08
correct_first = 1.0 - 0.9**10
correct_second = 1.0 - 0.95**10

VMEM_LIMIT = 56 * 1024 * 1024
MESH = pl.DeviceIdType.MESH
F32 = jnp.float32

DIMS = (("x", "z", "y"), ("y", "x", "z"), ("z", "y", "x"))
PARTS = (((0, 0, 16, 0), (3, 0, 8, 16)), ((1, 0, 16, 0), (3, 8, 8, 16)), ((2, 0, 16, 0),))
ROWS = (24, 24, 16)
W = 128
OWN = 4
SENT = 2
DIRECT = (STEPS - 1,)


def adamw(grad, param, moment, second):
    moment_new = beta_first * moment + (1.0 - beta_first) * grad
    second_new = beta_second * second + (1.0 - beta_second) * grad * grad
    ratio = moment_new / correct_first / (jnp.sqrt(second_new / correct_second) + epsilon)
    param_new = param - step_rate * (ratio + decay_rate * param)
    return (param_new, moment_new, second_new)


def scratch():
    tree = {
        "acts": pltpu.VMEM((16, 1024, BLOCK_ROWS), jnp.bfloat16),
        "grads0": pltpu.VMEM((2, 1024, HALF), jnp.bfloat16),
        "grads1": pltpu.VMEM((2, 1024, HALF), jnp.bfloat16),
        "turned": pltpu.VMEM((BLOCK_ROWS, 1024), jnp.bfloat16),
        "out": pltpu.VMEM((BUCKETS, 2, 2, 4, 16, HALF), F32),
        "rt": pltpu.VMEM((2, 4, 2, 1, 2048), F32),
        "rx": pltpu.VMEM((4, 2, 1, 2048), F32),
        "rxx": pltpu.VMEM((3, 2, 1, 2048), F32),
        "rxy": pltpu.VMEM((4, 1, 2048), F32),
        "rxz": pltpu.VMEM((4, 1, 2048), F32),
        "ry": pltpu.VMEM((2, 1, 2048), F32),
        "load_sem": pltpu.SemaphoreType.DMA((20,)),
        "state_sem": pltpu.SemaphoreType.DMA((3,)),
        "x_send": pltpu.SemaphoreType.DMA((STEPS, 3)),
        "x_recv": pltpu.SemaphoreType.DMA((STEPS, 3)),
        "p1_send": pltpu.SemaphoreType.DMA((STEPS, 3, 6)),
        "p1_recv": pltpu.SemaphoreType.DMA((STEPS, 3, 6)),
        "p2_send": pltpu.SemaphoreType.DMA((STEPS, 3, 6)),
        "p2_recv": pltpu.SemaphoreType.DMA((STEPS, 3, 6)),
        "p3_send": pltpu.SemaphoreType.DMA((STEPS, 3, 3)),
        "p3_recv": pltpu.SemaphoreType.DMA((STEPS, 3, 3)),
        "ag_send": pltpu.SemaphoreType.DMA((STEPS, 5)),
        "ag_recv": pltpu.SemaphoreType.DMA((STEPS, 5)),
        "d_send": pltpu.SemaphoreType.DMA((STEPS, 7)),
        "d_recv": pltpu.SemaphoreType.DMA((STEPS, 7)),
        "r_send": pltpu.SemaphoreType.DMA((10,)),
        "r_recv": pltpu.SemaphoreType.DMA((10,)),
    }
    for q in range(3):
        r = ROWS[q]
        tree[f"own{q}"] = pltpu.VMEM((OWN, 4, 4, 4, r, W), F32)
        tree[f"sent{q}"] = pltpu.VMEM((SENT, 4, 4, 4, r, W), F32)
        tree[f"xr{q}"] = pltpu.VMEM((4, 4, 4, 4, r, W), F32)
        tree[f"ra{q}"] = pltpu.VMEM((4, 6, 2, 4, r, W), F32)
        tree[f"q{q}"] = pltpu.VMEM((STEPS, 4, 4, r, W), F32)
        tree[f"rb{q}"] = pltpu.VMEM((STEPS, 12, r, W), F32)
        tree[f"rc{q}"] = pltpu.VMEM((STEPS, 3, r, W), F32)
    return tree


def kernel(names, order, logits, acts_hbm, keys_hbm, values_hbm, *refs):
    state_hbm, router_state = refs[0:3], refs[3:6]
    state, router_new = refs[6:9], refs[9:12]
    refs = refs[12:]
    ref = dict(zip(names, refs))
    rep = lax.axis_index("rep")
    inst = lax.axis_index("inst")
    yl, z = rep // 4, rep % 4
    yh, x, core = inst // 8, (inst // 2) % 4, inst % 2
    place = {"x": x, "y": yh * 2 + yl, "z": z, "c": core}

    def device(**change):
        at = {**place, **change}
        y = at["y"]
        return {"rep": (y % 2) * 4 + at["z"], "inst": ((y // 2) * 4 + at["x"]) * 2 + at["c"]}

    def along(dim, delta):
        return device(**{dim: (place[dim] + delta) % 4})

    sibling = device(c=1 - core)
    partner = device(y=yh * 2 + (1 - yl))

    def send(src, dst, send_sem, recv_sem, to):
        copy = pltpu.make_async_remote_copy(
            src_ref=src, dst_ref=dst, send_sem=send_sem, recv_sem=recv_sem, device_id=to, device_id_type=MESH
        )
        copy.start()

    def wait_recv(dst, sem):
        pltpu.make_async_copy(dst, dst, sem).wait()

    wait_send = wait_recv

    def grad_loads(half):
        return [
            pltpu.make_async_copy(
                part.at[:, half * HALF : (half + 1) * HALF],
                ref[f"grads{half}"].at[n],
                ref["load_sem"].at[16 + half * 2 + n],
            )
            for n, part in enumerate((keys_hbm, values_hbm))
        ]

    loads = grad_loads(0)
    for i in range(16):
        loads.append(
            pltpu.make_async_copy(
                acts_hbm.at[:, i * BLOCK_ROWS : (i + 1) * BLOCK_ROWS], ref["acts"].at[i], ref["load_sem"].at[i]
            )
        )
    late_loads = grad_loads(1)
    for load in loads + late_loads:
        load.start()
    state_loads = [pltpu.make_async_copy(state_hbm[n], state[n], ref["state_sem"].at[n]) for n in range(3)]

    barrier = pltpu.get_barrier_semaphore()
    peers = [sibling] + [along(d, delta) for d in "xyz" for delta in (1, 2, 3)]
    for peer in peers:
        pl.semaphore_signal(barrier, inc=1, device_id=peer, device_id_type=MESH)

    def router_term():
        for i in range(16):
            term = jnp.dot(logits[...], ref["acts"][i], preferred_element_type=F32)
            for e in range(8):
                ref["rt"][i // 8, e % 4, e // 4, :, pl.ds((i % 8) * 256, 256)] = term[e : e + 1, :]

    def spots(q, slot_y, slot_x):
        pair, every = pl.ds(slot_y * 2, 2), pl.ds(0, 4)
        return ((slot_x, every, pair), (pair, slot_x, every), (every, pair, slot_x))[q]

    def exchange(step, j):
        for q in range(3):
            spot = spots(q, j // 4, j % 4)
            send(
                ref[f"sent{q}"].at[(step % SENT,) + spot],
                ref[f"xr{q}"].at[(step % 4,) + spot],
                ref["x_send"].at[step, q],
                ref["x_recv"].at[step, q],
                sibling,
            )

    def matmul(step, first, last):
        bucket, par = step // 2, step % 2

        def body(j, carry):
            slot_y, slot_x = j // 4, j % 4
            block = order[bucket * 8 + j]
            for h, side in enumerate((core, 1 - core)):
                columns = ref["acts"][block % 16, :, pl.ds(pl.multiple_of(side * 128, 128), 128)]
                ref["turned"][h * 128 : (h + 1) * 128] = columns.T
            for n in range(2):
                lo = n * 256
                piece = jnp.dot(
                    ref["turned"][...],
                    ref[f"grads{par}"][block // 16, :, lo : lo + 256],
                    preferred_element_type=F32,
                )
                for h in range(2):
                    dst = "sent" if h else "own"
                    slot = step % (SENT if h else OWN)
                    for q in range(3):
                        for chunk, top, count, row in PARTS[q]:
                            if chunk // 2 != n:
                                continue
                            left = chunk % 2 * W
                            for l in range(2):
                                y = slot_y * 2 + l
                                for k in range(4):
                                    start = h * 128 + l * 64 + k * 16 + top
                                    value = piece[start : start + count, left : left + W]
                                    at = ((slot_x, k, y), (y, slot_x, k), (k, y, slot_x))[q]
                                    ref[f"{dst}{q}"][(slot,) + at + (pl.ds(row, count),)] = value

            @pl.when(j > first)
            def _():
                exchange(step, j - 1)

            return carry

        lax.fori_loop(first, last, body, 0)
        exchange(step, last - 1)

    def add_sibling(step):
        for q in range(3):
            own, xr = ref[f"own{q}"], ref[f"xr{q}"]
            wait_recv(xr.at[step % 4], ref["x_recv"].at[step, q])

            def body(d, carry):
                own[step % OWN, d] = own[step % OWN, d] + xr[step % 4, d]
                return carry

            lax.fori_loop(0, 4, body, 0)

    def views(step, q, phase):
        slot = step % OWN if phase == 1 else step
        src, recv = (ref[f"own{q}"], ref[f"ra{q}"]) if phase == 1 else (ref[f"q{q}"], ref[f"rb{q}"])
        at = lambda d, h: (slot, d, pl.ds(2 * h, 2))
        into = (lambda m: (step % 4, m)) if phase == 1 else (lambda m: (step, pl.ds(2 * m, 2)))
        return src, at, recv, into

    def ring_send(step, q, phase, m, where, delta):
        src, at, recv, into = views(step, q, phase)
        dim = DIMS[q][phase - 1]
        d, h = where
        send(
            src.at[at((place[dim] + d) % 4, h)],
            recv.at[into(m)],
            ref[f"p{phase}_send"].at[step, q, m],
            ref[f"p{phase}_recv"].at[step, q, m],
            along(dim, delta),
        )

    def ring_start(step, phase):
        for q in range(3):
            ring_send(step, q, phase, 0, (2, 0), 1)
            ring_send(step, q, phase, 1, (2, 1), 3)

    def ring_next(step, phase):
        for q in range(3):
            ring_send(step, q, phase, 2, (1, 1), 1)
            ring_send(step, q, phase, 3, (3, 0), 3)

    def ring_relay(step, phase):
        for q in range(3):
            src, at, recv, into = views(step, q, phase)
            here = place[DIMS[q][phase - 1]]
            for m, d, h in ((0, 1, 0), (1, 3, 1)):
                wait_recv(recv.at[into(m)], ref[f"p{phase}_recv"].at[step, q, m])
                spot = at((here + d) % 4, h)
                src[spot] = src[spot] + recv[into(m)]
                ring_send(step, q, phase, 4 + m, (d, h), d)

    def ring_end(step, phase):
        for q in range(3):
            src, at, recv, into = views(step, q, phase)
            here = place[DIMS[q][phase - 1]]
            for h, arrived in ((0, (3, 4)), (1, (2, 5))):
                for m in arrived:
                    wait_recv(recv.at[into(m)], ref[f"p{phase}_recv"].at[step, q, m])
                spot = at(here, h)
                total = src[spot] + recv[into(arrived[0])] + recv[into(arrived[1])]
                if phase == 1:
                    ref[f"q{q}"][step, pl.ds(2 * h, 2)] = total
                else:
                    src[spot] = total

    def ring_sent(step, phase):
        for q in range(3):
            _, _, recv, into = views(step, q, phase)
            for m in range(6):
                wait_send(recv.at[into(m)], ref[f"p{phase}_send"].at[step, q, m])

    def second_start(step):
        for m, delta in enumerate((2, 1, 3)):
            for q in range(3):
                dim = DIMS[q][1]
                send(
                    ref[f"q{q}"].at[step, (place[dim] + delta) % 4],
                    ref[f"rb{q}"].at[step, pl.ds(4 * m, 4)],
                    ref["p2_send"].at[step, q, m],
                    ref["p2_recv"].at[step, q, m],
                    along(dim, delta),
                )

    def second_end(step):
        for q in range(3):
            rb, here = ref[f"rb{q}"], place[DIMS[q][1]]
            for m in range(3):
                wait_recv(rb.at[step, pl.ds(4 * m, 4)], ref["p2_recv"].at[step, q, m])
            total = ref[f"q{q}"][step, here]
            for m in range(3):
                total = total + rb[step, pl.ds(4 * m, 4)]
            ref[f"q{q}"][step, here] = total

    def second_sent(step):
        for q in range(3):
            for m in range(3):
                wait_send(ref[f"rb{q}"].at[step, pl.ds(4 * m, 4)], ref["p2_send"].at[step, q, m])

    def exchange_sent(step):
        for q in range(3):
            wait_send(ref[f"xr{q}"].at[step % 4], ref["x_send"].at[step, q])

    def last_start(step):
        for q in range(3):
            second, third = DIMS[q][1:]
            for m in range(3):
                delta = (1, 3, 2)[m]
                send(
                    ref[f"q{q}"].at[step, place[second], (place[third] + delta) % 4],
                    ref[f"rc{q}"].at[step, m],
                    ref["p3_send"].at[step, q, m],
                    ref["p3_recv"].at[step, q, m],
                    along(third, delta),
                )

    def last_end(step):
        b, par = step // 2, step % 2
        for q in range(3):
            second, third = DIMS[q][1:]
            rc = ref[f"rc{q}"]
            for m in range(3):
                wait_recv(rc.at[step, m], ref["p3_recv"].at[step, q, m])
            total = ref[f"q{q}"][step, place[second], place[third]] + rc[step, 0] + rc[step, 1] + rc[step, 2]
            for chunk, top, count, row in PARTS[q]:
                ref["out"][b, par, yl, z, pl.ds(top, count), pl.ds(chunk * W, W)] = total[row : row + count]

    def last_sent(step):
        for q in range(3):
            for m in range(3):
                wait_send(ref[f"rc{q}"].at[step, m], ref["p3_send"].at[step, q, m])

    def gather_send(step, n, spot, to):
        out = ref["out"].at[(step // 2, step % 2) + spot]
        send(out, out, ref["ag_send"].at[step, n], ref["ag_recv"].at[step, n], to)

    def gather_wait(step, n, spot, which="ag_recv"):
        wait_recv(ref["out"].at[(step // 2, step % 2) + spot], ref[which].at[step, n])

    both = pl.ds(0, 2)

    def gather_partner(step):
        gather_send(step, 0, (yl, z), partner)

    def gather_start(step):
        gather_wait(step, 0, (1 - yl, z))
        gather_send(step, 1, (both, z), along("z", 1))
        gather_send(step, 2, (both, z), along("z", 3))

    def gather_relay(step):
        gather_wait(step, 1, (both, (z + 3) % 4))
        gather_send(step, 3, (0, (z + 3) % 4), along("z", 1))
        gather_wait(step, 2, (both, (z + 1) % 4))
        gather_send(step, 4, (1, (z + 1) % 4), along("z", 3))

    def gather_direct(step):
        b, par = step // 2, step % 2
        own = ref["out"].at[b, par, yl, z]
        for n in (5, 1, 6, 2, 4, 0, 3):
            dy, dz = divmod(n + 1, 4)
            to = device(y=yh * 2 + (yl + dy) % 2, z=(z + dz) % 4)
            send(own, own, ref["d_send"].at[step, n], ref["d_recv"].at[step, n], to)

    def gather_end(step):
        if step in DIRECT:
            for n in range(7):
                dy, dz = divmod(n + 1, 4)
                there = ref["out"].at[step // 2, step % 2, (yl + dy) % 2, (z - dz) % 4]
                wait_recv(there, ref["d_recv"].at[step, n])
        else:
            gather_wait(step, 3, (0, (z + 2) % 4))
            gather_wait(step, 4, (1, (z + 2) % 4))
        b, par = step // 2, step % 2
        columns = pl.ds(par * HALF, HALF)

        def body(i, carry):
            rows = pl.ds(pl.multiple_of(i * 16, 16), 16)
            grad = ref["out"][b, par, i // 4, i % 4]
            fresh = adamw(grad, *(part[b, rows, columns] for part in state))
            for part, value in zip(state, fresh):
                part[b, rows, columns] = value
            return carry

        lax.fori_loop(0, 8, body, 0)

    def gather_sent(step):
        if step in DIRECT:
            for n in range(7):
                wait_send(ref["out"].at[step // 2, step % 2, yl, z], ref["d_send"].at[step, n])
            return
        for n, spot in enumerate(((yl, z), (both, z), (both, z), (0, z), (1, z))):
            gather_wait(step, n, spot, "ag_send")

    def state_start():
        for load in state_loads:
            load.start()

    def state_end():
        for load in state_loads:
            load.wait()

    def router_send(n, src, dst, to):
        send(src, dst, ref["r_send"].at[n], ref["r_recv"].at[n], to)

    def router_wait(n, dst):
        wait_recv(dst, ref["r_recv"].at[n])

    def router_0():
        router_send(0, ref["rt"].at[1 - core], ref["rx"], sibling)

    def router_1():
        router_wait(0, ref["rx"])
        ref["rt"][core] = ref["rt"][core] + ref["rx"][...]
        for m, delta in enumerate((1, 2, 3)):
            router_send(1 + m, ref["rt"].at[core, (x + delta) % 4], ref["rxx"].at[m], along("x", delta))

    def router_2():
        for m in range(3):
            router_wait(1 + m, ref["rxx"].at[m])
        ref["ry"][...] = ref["rt"][core, x] + ref["rxx"][0] + ref["rxx"][1] + ref["rxx"][2]
        here = place["y"]
        ref["rxy"][here] = ref["ry"][yh]
        for m, delta in enumerate((1, 2, 3)):
            to = (here + delta) % 4
            router_send(4 + m, ref["ry"].at[to // 2], ref["rxy"].at[here], along("y", delta))

    def router_3():
        here = place["y"]
        for m, delta in enumerate((1, 2, 3)):
            router_wait(4 + m, ref["rxy"].at[(here - delta) % 4])
        total = ref["rxy"][0] + ref["rxy"][1] + ref["rxy"][2] + ref["rxy"][3]
        ref["rxz"][z] = total
        for m, delta in enumerate((1, 2, 3)):
            router_send(7 + m, ref["rxz"].at[z], ref["rxz"].at[z], along("z", delta))

    def router_4():
        for m, delta in enumerate((1, 2, 3)):
            router_wait(7 + m, ref["rxz"].at[(z - delta) % 4])
        total = ref["rxz"][0] + ref["rxz"][1] + ref["rxz"][2] + ref["rxz"][3]
        for row in range(2):
            at = pl.ds(row, 1)
            fresh = adamw(total[:, row * 1024 : (row + 1) * 1024], *(part[at] for part in router_state))
            for part, value in zip(router_new, fresh):
                part[at] = value

    def router_sent():
        wait_send(ref["rx"], ref["r_send"].at[0])
        for m in range(3):
            wait_send(ref["rxx"].at[m], ref["r_send"].at[1 + m])
            wait_send(ref["rxy"].at[m], ref["r_send"].at[4 + m])
            wait_send(ref["rxz"].at[m], ref["r_send"].at[7 + m])

    router_stages = {0: router_0, 1: router_1, 2: router_2, 3: router_3, 4: router_4}

    def run(stage, *args):
        with jax.named_scope(f"{stage.__name__}#s={'_'.join(map(str, args))}"):
            stage(*args)

    def live(step):
        return 0 <= step < STEPS

    with jax.named_scope("loads"):
        for load in loads:
            load.wait()
    with jax.named_scope("barrier"):
        pl.semaphore_wait(barrier, len(peers))
    run(matmul, 0, 0, 8)
    run(router_term)
    run(router_0)
    run(add_sibling, 0)
    run(ring_start, 0, 1)
    for load in late_loads:
        load.wait()
    state_start()

    def all_sent(step):
        if step in DIRECT:
            second_sent(step)
        else:
            ring_sent(step, 2)
        last_sent(step)
        gather_sent(step)

    for i in range(STEPS + 5):
        if live(i - 2) and i - 2 not in DIRECT:
            run(ring_relay, i - 2, 2)
        if live(i):
            run(ring_next, i, 1)
        if live(i + 1):
            if live(i - 1):
                run(exchange_sent, i - 1)
            if live(i - 3):
                run(ring_sent, i - 3, 1)
            run(matmul, i + 1, 0, 4)
        if live(i - 1):
            run(ring_end, i - 1, 1)
            if i - 1 in DIRECT:
                run(second_start, i - 1)
            else:
                run(ring_start, i - 1, 2)
                run(ring_next, i - 1, 2)
        if live(i + 1):
            run(matmul, i + 1, 4, 8)
        if live(i):
            run(ring_relay, i, 1)
        if live(i - 2):
            if i - 2 in DIRECT:
                run(second_end, i - 2)
            else:
                run(ring_end, i - 2, 2)
            run(last_start, i - 2)
        if live(i + 1):
            run(add_sibling, i + 1)
            run(ring_start, i + 1, 1)
        if live(i - 3):
            run(last_end, i - 3)
            if i - 3 in DIRECT:
                run(gather_direct, i - 3)
            else:
                run(gather_partner, i - 3)
        if live(i - 4) and i - 4 not in DIRECT:
            run(gather_start, i - 4)
        if live(i - 5) and i - 5 not in DIRECT:
            run(gather_relay, i - 5)
        if i + 1 in router_stages:
            run(router_stages[i + 1])
        if i == 5:
            run(state_end)
        if live(i - 6):
            run(gather_end, i - 6)
            run(all_sent, i - 6)
    run(gather_end, STEPS - 1)
    with jax.named_scope("ending"):
        for step in range(STEPS - 4, STEPS):
            if step >= STEPS - 2:
                exchange_sent(step)
            ring_sent(step, 1)
        all_sent(STEPS - 1)
        router_sent()


def on_device(
    acts,
    grad_keys,
    grad_values,
    grad_logits,
    order,
    bucket_param,
    bucket_m,
    bucket_v,
    router_param,
    router_m,
    router_v,
):
    tree = scratch()
    names = tuple(tree)
    hbm, vmem = pl.BlockSpec(memory_space=pltpu.HBM), pl.BlockSpec(memory_space=pltpu.VMEM)
    fresh = pl.pallas_call(
        lambda *refs: kernel(names, *refs),
        out_shape=tuple(
            pltpu.VMEM(part.shape, F32) for part in (bucket_param, bucket_m, bucket_v, router_param, router_m, router_v)
        ),
        in_specs=[pl.BlockSpec(memory_space=pltpu.SMEM), vmem] + [hbm] * 6 + [vmem] * 3,
        out_specs=(vmem,) * 6,
        scratch_shapes=list(tree.values()),
        compiler_params=pltpu.CompilerParams(
            collective_id=0, has_side_effects=True, vmem_limit_bytes=VMEM_LIMIT
        ),
        cost_estimate=pl.CostEstimate(flops=17_200_000_000, bytes_accessed=24_000_000, transcendentals=0),
        name="reduce",
    )(
        order,
        grad_logits,
        acts,
        grad_keys,
        grad_values,
        bucket_param,
        bucket_m,
        bucket_v,
        router_param,
        router_m,
        router_v,
    )
    return pl.pallas_call(
        store,
        out_shape=tuple(jax.ShapeDtypeStruct(part.shape, F32) for part in fresh),
        in_specs=[vmem] * 6,
        out_specs=(hbm,) * 6,
        scratch_shapes=[pltpu.SemaphoreType.DMA((6,))],
        compiler_params=pltpu.CompilerParams(vmem_limit_bytes=1024 * 1024),
        name="store",
    )(*(pltpu.with_memory_space_constraint(part, pltpu.VMEM) for part in fresh))


def store(*refs):
    copies = [pltpu.make_async_copy(refs[n], refs[6 + n], refs[12].at[n]) for n in range(6)]
    for copy in copies:
        copy.start()
    for copy in copies:
        copy.wait()


def solution(mesh):
    state, router = P(None, "inst", None), P("inst", None)
    tokens = P(("rep", "inst"), None)
    return jax.shard_map(
        on_device,
        mesh=mesh,
        in_specs=(tokens, tokens, tokens, P(None, ("rep", "inst")), P(), state, state, state, router, router, router),
        out_specs=(state, state, state, router, router, router),
        check_vma=False,
    )
```

```python
import jax
import jax.numpy as jnp
from jax import lax
from jax.experimental import pallas as pl
from jax.experimental.pallas import tpu as pltpu
from jax.sharding import PartitionSpec as P

BUCKETS = 4
BLOCK_ROWS = 256
STEPS = 8
HALF = 512

beta_first = 0.9
beta_second = 0.95
step_rate = 0.05
decay_rate = 0.1
epsilon = 1e-08
correct_first = 1.0 - 0.9**10
correct_second = 1.0 - 0.95**10

VMEM_LIMIT = 56 * 1024 * 1024
MESH = pl.DeviceIdType.MESH
F32 = jnp.float32

DIMS = (("x", "z", "y"), ("y", "x", "z"), ("z", "y", "x"))
PARTS = (((0, 0, 16, 0), (3, 0, 8, 16)), ((1, 0, 16, 0), (3, 8, 8, 16)), ((2, 0, 16, 0),))
ROWS = (24, 24, 16)
W = 128
OWN = 4
SENT = 2
RING = 4
DIRECT = (STEPS - 1,)
DIRECT_GATHER = (STEPS - 3, STEPS - 2, STEPS - 1)


def adamw(grad, param, moment, second):
    moment_new = beta_first * moment + (1.0 - beta_first) * grad
    second_new = beta_second * second + (1.0 - beta_second) * grad * grad
    ratio = moment_new / correct_first / (jnp.sqrt(second_new / correct_second) + epsilon)
    param_new = param - step_rate * (ratio + decay_rate * param)
    return (param_new, moment_new, second_new)


def scratch():
    tree = {
        "acts": pltpu.VMEM((16, 1024, BLOCK_ROWS), jnp.bfloat16),
        "grads0": pltpu.VMEM((2, 1024, HALF), jnp.bfloat16),
        "grads1": pltpu.VMEM((2, 1024, HALF), jnp.bfloat16),
        "turned0": pltpu.VMEM((BLOCK_ROWS, 1024), jnp.bfloat16),
        "turned1": pltpu.VMEM((BLOCK_ROWS, 1024), jnp.bfloat16),
        "out": pltpu.VMEM((BUCKETS, 2, 2, 4, 16, HALF), F32),
        "rt": pltpu.VMEM((2, 4, 2, 1, 2048), F32),
        "rx": pltpu.VMEM((4, 2, 1, 2048), F32),
        "rxx": pltpu.VMEM((3, 2, 1, 2048), F32),
        "rxy": pltpu.VMEM((4, 1, 2048), F32),
        "rxz": pltpu.VMEM((4, 1, 2048), F32),
        "ry": pltpu.VMEM((2, 1, 2048), F32),
        "load_sem": pltpu.SemaphoreType.DMA((3,)),
        "state_sem": pltpu.SemaphoreType.DMA((3,)),
        "x_send": pltpu.SemaphoreType.DMA((SENT, 3)),
        "x_recv": pltpu.SemaphoreType.DMA((SENT, 3)),
        "p1_send": pltpu.SemaphoreType.DMA((RING, 3)),
        "p1_recv": pltpu.SemaphoreType.DMA((RING, 3, 2)),
        "p2_send": pltpu.SemaphoreType.DMA((RING, 3)),
        "p2_recv": pltpu.SemaphoreType.DMA((RING, 3, 2)),
        "p3_send": pltpu.SemaphoreType.DMA((RING, 3)),
        "p3_recv": pltpu.SemaphoreType.DMA((RING, 3)),
        "ag_send": pltpu.SemaphoreType.DMA((RING, 3)),
        "ag_recv": pltpu.SemaphoreType.DMA((RING, 5)),
        "d_recv": pltpu.SemaphoreType.DMA((3, 7)),
        "r_send": pltpu.SemaphoreType.DMA((4,)),
        "r_recv": pltpu.SemaphoreType.DMA((8,)),
    }
    for q in range(3):
        r = ROWS[q]
        tree[f"own{q}"] = pltpu.VMEM((OWN, 4, 4, 4, r, W), F32)
        tree[f"sent{q}"] = pltpu.VMEM((SENT, 4, 4, 4, r, W), F32)
        tree[f"xr{q}"] = pltpu.VMEM((4, 4, 4, 4, r, W), F32)
        tree[f"ra{q}"] = pltpu.VMEM((4, 6, 2, 4, r, W), F32)
        tree[f"q{q}"] = pltpu.VMEM((STEPS, 4, 4, r, W), F32)
        tree[f"rb{q}"] = pltpu.VMEM((STEPS, 12, r, W), F32)
        tree[f"rc{q}"] = pltpu.VMEM((STEPS, 3, r, W), F32)
    return tree


def kernel(names, order, logits, acts_hbm, keys_hbm, values_hbm, *refs):
    state_hbm, router_state = refs[0:3], refs[3:6]
    state, router_new = refs[6:9], refs[9:12]
    refs = refs[12:]
    ref = dict(zip(names, refs))
    rep = lax.axis_index("rep")
    inst = lax.axis_index("inst")
    yl, z = rep // 4, rep % 4
    yh, x, core = inst // 8, (inst // 2) % 4, inst % 2
    place = {"x": x, "y": yh * 2 + yl, "z": z, "c": core}

    def device(**change):
        at = {**place, **change}
        y = at["y"]
        return {"rep": (y % 2) * 4 + at["z"], "inst": ((y // 2) * 4 + at["x"]) * 2 + at["c"]}

    def along(dim, delta):
        return device(**{dim: (place[dim] + delta) % 4})

    sibling = device(c=1 - core)
    partner = device(y=yh * 2 + (1 - yl))

    def send(src, dst, send_sem, recv_sem, to):
        copy = pltpu.make_async_remote_copy(
            src_ref=src, dst_ref=dst, send_sem=send_sem, recv_sem=recv_sem, device_id=to, device_id_type=MESH
        )
        copy.start()

    def wait_recv(dst, sem):
        pltpu.make_async_copy(dst, dst, sem).wait()

    wait_send = wait_recv

    def grad_loads(half):
        return [
            pltpu.make_async_copy(
                part.at[:, half * HALF : (half + 1) * HALF],
                ref[f"grads{half}"].at[n],
                ref["load_sem"].at[1 + half],
            )
            for n, part in enumerate((keys_hbm, values_hbm))
        ]

    loads = grad_loads(0)
    for i in range(16):
        loads.append(
            pltpu.make_async_copy(
                acts_hbm.at[:, i * BLOCK_ROWS : (i + 1) * BLOCK_ROWS], ref["acts"].at[i], ref["load_sem"].at[0]
            )
        )
    late_loads = grad_loads(1)
    for load in loads + late_loads:
        load.start()
    state_loads = [pltpu.make_async_copy(state_hbm[n], state[n], ref["state_sem"].at[n]) for n in range(3)]

    barrier = pltpu.get_barrier_semaphore()
    peers = [sibling] + [along(d, delta) for d in "xyz" for delta in (1, 2, 3)]
    for peer in peers:
        pl.semaphore_signal(barrier, inc=1, device_id=peer, device_id_type=MESH)

    def router_term():
        for i in range(16):
            term = jnp.dot(logits[...], ref["acts"][i], preferred_element_type=F32)
            for e in range(8):
                ref["rt"][i // 8, e % 4, e // 4, :, pl.ds((i % 8) * 256, 256)] = term[e : e + 1, :]

    def spots(q, slot_y, slot_x):
        pair, every = pl.ds(slot_y * 2, 2), pl.ds(0, 4)
        return ((slot_x, every, pair), (pair, slot_x, every), (every, pair, slot_x))[q]

    def exchange(step, j):
        for q in range(3):
            spot = spots(q, j // 4, j % 4)
            send(
                ref[f"sent{q}"].at[(step % SENT,) + spot],
                ref[f"xr{q}"].at[(step % 4,) + spot],
                ref["x_send"].at[step % SENT, q],
                ref["x_recv"].at[step % SENT, q],
                sibling,
            )

    def turn(step, j, into):
        block = order[step // 2 * 8 + j] % 16
        for h, side in enumerate((core, 1 - core)):
            columns = ref["acts"][block, :, pl.ds(pl.multiple_of(side * 128, 128), 128)]
            into[h * 128 : (h + 1) * 128] = columns.T

    def matmul(step, first, last):
        bucket, par = step // 2, step % 2
        turn(step, first, ref["turned0"])

        def body(pair, carry):
            j = first + pair * 2

            @pl.when(pair > 0)
            def _():
                exchange(step, j - 1)

            dots(step, j, 0, j + 1)
            exchange(step, j)
            dots(step, j + 1, 1, jnp.minimum(j + 2, 7))
            return carry

        def dots(step, j, now, later):
            slot_y, slot_x = j // 4, j % 4
            block = order[bucket * 8 + j]
            turn(step, later, ref[f"turned{1 - now}"])
            for n in range(2):
                lo = n * 256
                piece = jnp.dot(
                    ref[f"turned{now}"][...],
                    ref[f"grads{par}"][block // 16, :, lo : lo + 256],
                    preferred_element_type=F32,
                )
                for h in range(2):
                    dst = "sent" if h else "own"
                    slot = step % (SENT if h else OWN)
                    for q in range(3):
                        for chunk, top, count, row in PARTS[q]:
                            if chunk // 2 != n:
                                continue
                            left = chunk % 2 * W
                            for l in range(2):
                                y = slot_y * 2 + l
                                for k in range(4):
                                    start = h * 128 + l * 64 + k * 16 + top
                                    value = piece[start : start + count, left : left + W]
                                    at = ((slot_x, k, y), (y, slot_x, k), (k, y, slot_x))[q]
                                    ref[f"{dst}{q}"][(slot,) + at + (pl.ds(row, count),)] = value

        lax.fori_loop(0, (last - first) // 2, body, 0)
        exchange(step, last - 1)

    def add_sibling(step):
        for q in range(3):
            own, xr = ref[f"own{q}"], ref[f"xr{q}"]
            wait_recv(xr.at[step % 4], ref["x_recv"].at[step % SENT, q])

            def body(d, carry):
                own[step % OWN, d] = own[step % OWN, d] + xr[step % 4, d]
                return carry

            lax.fori_loop(0, 4, body, 0)

    def views(step, q, phase):
        slot = step % OWN if phase == 1 else step
        src, recv = (ref[f"own{q}"], ref[f"ra{q}"]) if phase == 1 else (ref[f"q{q}"], ref[f"rb{q}"])
        at = lambda d, h: (slot, d, pl.ds(2 * h, 2))
        into = (lambda m: (step % 4, m)) if phase == 1 else (lambda m: (step, pl.ds(2 * m, 2)))
        return src, at, recv, into

    def group(step, phase, first, count):
        return (step % 4, pl.ds(first, count)) if phase == 1 else (step, pl.ds(2 * first, 2 * count))

    def ring_send(step, q, phase, m, where, delta):
        src, at, recv, into = views(step, q, phase)
        dim = DIMS[q][phase - 1]
        d, h = where
        send(
            src.at[at((place[dim] + d) % 4, h)],
            recv.at[into(m)],
            ref[f"p{phase}_send"].at[step % RING, q],
            ref[f"p{phase}_recv"].at[step % RING, q, int(m > 1)],
            along(dim, delta),
        )

    def ring_start(step, phase):
        for q in range(3):
            ring_send(step, q, phase, 0, (2, 0), 1)
            ring_send(step, q, phase, 1, (2, 1), 3)

    def ring_next(step, phase):
        for q in range(3):
            ring_send(step, q, phase, 2, (1, 1), 1)
            ring_send(step, q, phase, 3, (3, 0), 3)

    def ring_relay(step, phase):
        for q in range(3):
            src, at, recv, into = views(step, q, phase)
            here = place[DIMS[q][phase - 1]]
            wait_recv(recv.at[group(step, phase, 0, 2)], ref[f"p{phase}_recv"].at[step % RING, q, 0])
            for m, d, h in ((0, 1, 0), (1, 3, 1)):
                spot = at((here + d) % 4, h)
                src[spot] = src[spot] + recv[into(m)]
                ring_send(step, q, phase, 4 + m, (d, h), d)

    def ring_end(step, phase):
        for q in range(3):
            src, at, recv, into = views(step, q, phase)
            here = place[DIMS[q][phase - 1]]
            wait_recv(recv.at[group(step, phase, 2, 4)], ref[f"p{phase}_recv"].at[step % RING, q, 1])
            for h, arrived in ((0, (3, 4)), (1, (2, 5))):
                spot = at(here, h)
                total = src[spot] + recv[into(arrived[0])] + recv[into(arrived[1])]
                if phase == 1:
                    ref[f"q{q}"][step, pl.ds(2 * h, 2)] = total
                else:
                    src[spot] = total

    def ring_sent(step, phase):
        for q in range(3):
            recv = views(step, q, phase)[2]
            wait_send(recv.at[group(step, phase, 0, 6)], ref[f"p{phase}_send"].at[step % RING, q])

    def second_start(step):
        for m, delta in enumerate((2, 1, 3)):
            for q in range(3):
                dim = DIMS[q][1]
                send(
                    ref[f"q{q}"].at[step, (place[dim] + delta) % 4],
                    ref[f"rb{q}"].at[step, pl.ds(4 * m, 4)],
                    ref["p2_send"].at[step % RING, q],
                    ref["p2_recv"].at[step % RING, q, 0],
                    along(dim, delta),
                )

    def second_end(step):
        for q in range(3):
            rb, here = ref[f"rb{q}"], place[DIMS[q][1]]
            wait_recv(rb.at[step], ref["p2_recv"].at[step % RING, q, 0])
            total = ref[f"q{q}"][step, here]
            for m in range(3):
                total = total + rb[step, pl.ds(4 * m, 4)]
            ref[f"q{q}"][step, here] = total

    def exchange_sent(step):
        for q in range(3):
            wait_send(ref[f"xr{q}"].at[step % 4], ref["x_send"].at[step % SENT, q])

    def last_start(step):
        for q in range(3):
            second, third = DIMS[q][1:]
            for m in range(3):
                delta = (1, 3, 2)[m]
                send(
                    ref[f"q{q}"].at[step, place[second], (place[third] + delta) % 4],
                    ref[f"rc{q}"].at[step, m],
                    ref["p3_send"].at[step % RING, q],
                    ref["p3_recv"].at[step % RING, q],
                    along(third, delta),
                )

    def last_end(step):
        b, par = step // 2, step % 2
        for q in range(3):
            second, third = DIMS[q][1:]
            rc = ref[f"rc{q}"]
            wait_recv(rc.at[step], ref["p3_recv"].at[step % RING, q])
            total = ref[f"q{q}"][step, place[second], place[third]] + rc[step, 0] + rc[step, 1] + rc[step, 2]
            for chunk, top, count, row in PARTS[q]:
                ref["out"][b, par, yl, z, pl.ds(top, count), pl.ds(chunk * W, W)] = total[row : row + count]

    def last_sent(step):
        for q in range(3):
            wait_send(ref[f"rc{q}"].at[step], ref["p3_send"].at[step % RING, q])

    def gather_send(step, n, spot, to):
        out = ref["out"].at[(step // 2, step % 2) + spot]
        send(out, out, ref["ag_send"].at[step % RING, (n + 1) // 2], ref["ag_recv"].at[step % RING, n], to)

    def gather_wait(step, n, spot):
        wait_recv(ref["out"].at[(step // 2, step % 2) + spot], ref["ag_recv"].at[step % RING, n])

    both = pl.ds(0, 2)

    def gather_partner(step):
        gather_send(step, 0, (yl, z), partner)

    def gather_start(step):
        gather_wait(step, 0, (1 - yl, z))
        gather_send(step, 1, (both, z), along("z", 1))
        gather_send(step, 2, (both, z), along("z", 3))

    def gather_relay(step):
        gather_wait(step, 1, (both, (z + 3) % 4))
        gather_send(step, 3, (0, (z + 3) % 4), along("z", 1))
        gather_wait(step, 2, (both, (z + 1) % 4))
        gather_send(step, 4, (1, (z + 1) % 4), along("z", 3))

    def gather_direct(step):
        b, par = step // 2, step % 2
        own = ref["out"].at[b, par, yl, z]
        for count, n in enumerate((5, 1, 6, 2, 4, 0, 3)):
            dy, dz = divmod(n + 1, 4)
            to = device(y=yh * 2 + (yl + dy) % 2, z=(z + dz) % 4)
            sent = (0, 1, 1, 1, 1, 2, 2)[count]
            send(own, own, ref["ag_send"].at[step % RING, sent], ref["d_recv"].at[STEPS - 1 - step, n], to)

    def gather_end(step):
        if step in DIRECT_GATHER:
            for n in range(7):
                dy, dz = divmod(n + 1, 4)
                there = ref["out"].at[step // 2, step % 2, (yl + dy) % 2, (z - dz) % 4]
                wait_recv(there, ref["d_recv"].at[STEPS - 1 - step, n])
        else:
            gather_wait(step, 3, (0, (z + 2) % 4))
            gather_wait(step, 4, (1, (z + 2) % 4))
        b, par = step // 2, step % 2
        columns = pl.ds(par * HALF, HALF)

        def body(i, carry):
            rows = pl.ds(pl.multiple_of(i * 16, 16), 16)
            grad = ref["out"][b, par, i // 4, i % 4]
            fresh = adamw(grad, *(part[b, rows, columns] for part in state))
            for part, value in zip(state, fresh):
                part[b, rows, columns] = value
            return carry

        lax.fori_loop(0, 8, body, 0)

    def gather_sent(step):
        out = ref["out"].at[step // 2, step % 2]
        for n, part in enumerate((out.at[0, 0], out.at[0], out.at[both, 0])):
            wait_send(part, ref["ag_send"].at[step % RING, n])

    def state_start():
        for load in state_loads:
            load.start()

    def state_end():
        for load in state_loads:
            load.wait()

    def router_send(n, src, dst, to):
        send(src, dst, ref["r_send"].at[(n + 2) // 3], ref["r_recv"].at[max(n - 2, min(n, 1))], to)

    def router_wait(n, dst):
        wait_recv(dst, ref["r_recv"].at[max(n - 2, min(n, 1))])

    def router_0():
        router_send(0, ref["rt"].at[1 - core], ref["rx"], sibling)

    def router_1():
        router_wait(0, ref["rx"])
        ref["rt"][core] = ref["rt"][core] + ref["rx"][...]
        for m, delta in enumerate((1, 2, 3)):
            router_send(1 + m, ref["rt"].at[core, (x + delta) % 4], ref["rxx"].at[m], along("x", delta))

    def router_2():
        router_wait(1, ref["rxx"])
        ref["ry"][...] = ref["rt"][core, x] + ref["rxx"][0] + ref["rxx"][1] + ref["rxx"][2]
        here = place["y"]
        ref["rxy"][here] = ref["ry"][yh]
        for m, delta in enumerate((1, 2, 3)):
            to = (here + delta) % 4
            router_send(4 + m, ref["ry"].at[to // 2], ref["rxy"].at[here], along("y", delta))

    def router_3():
        here = place["y"]
        for m, delta in enumerate((1, 2, 3)):
            router_wait(4 + m, ref["rxy"].at[(here - delta) % 4])
        total = ref["rxy"][0] + ref["rxy"][1] + ref["rxy"][2] + ref["rxy"][3]
        ref["rxz"][z] = total
        for m, delta in enumerate((1, 2, 3)):
            router_send(7 + m, ref["rxz"].at[z], ref["rxz"].at[z], along("z", delta))

    def router_4():
        for m, delta in enumerate((1, 2, 3)):
            router_wait(7 + m, ref["rxz"].at[(z - delta) % 4])
        total = ref["rxz"][0] + ref["rxz"][1] + ref["rxz"][2] + ref["rxz"][3]
        for row in range(2):
            at = pl.ds(row, 1)
            fresh = adamw(total[:, row * 1024 : (row + 1) * 1024], *(part[at] for part in router_state))
            for part, value in zip(router_new, fresh):
                part[at] = value

    def router_sent():
        wait_send(ref["rx"], ref["r_send"].at[0])
        wait_send(ref["rxx"], ref["r_send"].at[1])
        wait_send(ref["rxy"].at[pl.ds(0, 3)], ref["r_send"].at[2])
        wait_send(ref["rxz"].at[pl.ds(0, 3)], ref["r_send"].at[3])

    router_stages = {0: router_0, 1: router_1, 2: router_2, 3: router_3, 4: router_4}

    def run(stage, *args):
        with jax.named_scope(f"{stage.__name__}#s={'_'.join(map(str, args))}"):
            stage(*args)

    def live(step):
        return 0 <= step < STEPS

    with jax.named_scope("loads"):
        wait_recv(ref["grads0"], ref["load_sem"].at[1])
        wait_recv(ref["acts"], ref["load_sem"].at[0])
    with jax.named_scope("barrier"):
        pl.semaphore_wait(barrier, len(peers))
    run(matmul, 0, 0, 8)
    run(add_sibling, 0)
    run(ring_start, 0, 1)

    def all_sent(step):
        gather_sent(step)

    for i in range(STEPS + 5):
        if live(i - 2) and i - 2 not in DIRECT:
            run(ring_relay, i - 2, 2)
        if live(i):
            run(ring_next, i, 1)
        if i == 0:
            run(router_term)
            run(router_0)
            wait_recv(ref["grads1"], ref["load_sem"].at[2])
            state_start()
        if live(i + 1):
            if live(i - 1):
                run(exchange_sent, i - 1)
            if live(i - 3):
                run(ring_sent, i - 3, 1)
            run(matmul, i + 1, 0, 4)
        if live(i - 1):
            run(ring_end, i - 1, 1)
            if i - 1 in DIRECT:
                run(second_start, i - 1)
            else:
                run(ring_start, i - 1, 2)
                run(ring_next, i - 1, 2)
        if live(i + 1):
            run(matmul, i + 1, 4, 8)
        if live(i):
            run(ring_relay, i, 1)
        if live(i - 2):
            if i - 2 in DIRECT:
                run(second_end, i - 2)
            else:
                run(ring_end, i - 2, 2)
            run(last_start, i - 2)
        if live(i + 1):
            run(add_sibling, i + 1)
            run(ring_start, i + 1, 1)
        if live(i - 3):
            run(last_end, i - 3)
            run(ring_sent, i - 3, 2)
            run(last_sent, i - 3)
            if i - 3 in DIRECT_GATHER:
                run(gather_direct, i - 3)
            else:
                run(gather_partner, i - 3)
        if live(i - 4) and i - 4 not in DIRECT_GATHER:
            run(gather_start, i - 4)
        if live(i - 5) and i - 5 not in DIRECT_GATHER:
            run(gather_relay, i - 5)
        if i + 1 in router_stages:
            run(router_stages[i + 1])
        if i == 5:
            run(state_end)
        if live(i - 6):
            run(gather_end, i - 6)
            run(all_sent, i - 6)
    run(gather_end, STEPS - 1)
    with jax.named_scope("ending"):
        for step in range(STEPS - 4, STEPS):
            if step >= STEPS - 2:
                exchange_sent(step)
            ring_sent(step, 1)
        all_sent(STEPS - 1)
        router_sent()


def on_device(
    acts,
    grad_keys,
    grad_values,
    grad_logits,
    order,
    bucket_param,
    bucket_m,
    bucket_v,
    router_param,
    router_m,
    router_v,
):
    tree = scratch()
    names = tuple(tree)
    hbm, vmem = pl.BlockSpec(memory_space=pltpu.HBM), pl.BlockSpec(memory_space=pltpu.VMEM)
    fresh = pl.pallas_call(
        lambda *refs: kernel(names, *refs),
        out_shape=tuple(
            pltpu.VMEM(part.shape, F32) for part in (bucket_param, bucket_m, bucket_v, router_param, router_m, router_v)
        ),
        in_specs=[pl.BlockSpec(memory_space=pltpu.SMEM), vmem] + [hbm] * 6 + [vmem] * 3,
        out_specs=(vmem,) * 6,
        scratch_shapes=list(tree.values()),
        compiler_params=pltpu.CompilerParams(
            collective_id=0, has_side_effects=True, vmem_limit_bytes=VMEM_LIMIT
        ),
        cost_estimate=pl.CostEstimate(flops=17_200_000_000, bytes_accessed=24_000_000, transcendentals=0),
        name="reduce",
    )(
        order,
        grad_logits,
        acts,
        grad_keys,
        grad_values,
        bucket_param,
        bucket_m,
        bucket_v,
        router_param,
        router_m,
        router_v,
    )
    return pl.pallas_call(
        store,
        out_shape=tuple(jax.ShapeDtypeStruct(part.shape, F32) for part in fresh),
        in_specs=[vmem] * 6,
        out_specs=(hbm,) * 6,
        scratch_shapes=[pltpu.SemaphoreType.DMA((6,))],
        compiler_params=pltpu.CompilerParams(vmem_limit_bytes=1024 * 1024),
        name="store",
    )(*(pltpu.with_memory_space_constraint(part, pltpu.VMEM) for part in fresh))


def store(*refs):
    copies = [pltpu.make_async_copy(refs[n], refs[6 + n], refs[12].at[n]) for n in range(6)]
    for copy in copies:
        copy.start()
    for copy in copies:
        copy.wait()


def solution(mesh):
    state, router = P(None, "inst", None), P("inst", None)
    tokens = P(("rep", "inst"), None)
    return jax.shard_map(
        on_device,
        mesh=mesh,
        in_specs=(tokens, tokens, tokens, P(None, ("rep", "inst")), P(), state, state, state, router, router, router),
        out_specs=(state, state, state, router, router, router),
        check_vma=False,
    )
```

```python
import jax
import jax.numpy as jnp
from jax import lax
from jax.experimental import pallas as pl
from jax.experimental.pallas import tpu as pltpu
from jax.sharding import PartitionSpec as P

BUCKETS = 4
BLOCK_ROWS = 256
STEPS = 8
HALF = 512
DEEP = 512

beta_first = 0.9
beta_second = 0.95
step_rate = 0.05
decay_rate = 0.1
epsilon = 1e-08
correct_first = 1.0 - 0.9**10
correct_second = 1.0 - 0.95**10

VMEM_LIMIT = 56 * 1024 * 1024
MESH = pl.DeviceIdType.MESH
F32 = jnp.float32

DIMS = (("x", "z", "y"), ("y", "x", "z"), ("z", "y", "x"))
PARTS = (((0, 0, 16, 0), (3, 0, 8, 16)), ((1, 0, 16, 0), (3, 8, 8, 16)), ((2, 0, 16, 0),))
ROWS = (24, 24, 16)
W = 128
OWN = 4
SENT = 2
RING = 4
DIRECT = (STEPS - 1,)
DIRECT_GATHER = (STEPS - 2, STEPS - 1)


def adamw(grad, param, moment, second):
    moment_new = beta_first * moment + (1.0 - beta_first) * grad
    second_new = beta_second * second + (1.0 - beta_second) * grad * grad
    ratio = moment_new / correct_first / (jnp.sqrt(second_new / correct_second) + epsilon)
    param_new = param - step_rate * (ratio + decay_rate * param)
    return (param_new, moment_new, second_new)


def scratch():
    tree = {
        "acts0": pltpu.VMEM((16, DEEP, BLOCK_ROWS), jnp.bfloat16),
        "acts1": pltpu.VMEM((16, DEEP, BLOCK_ROWS), jnp.bfloat16),
        "grads00": pltpu.VMEM((2, DEEP, HALF), jnp.bfloat16),
        "grads01": pltpu.VMEM((2, DEEP, HALF), jnp.bfloat16),
        "grads10": pltpu.VMEM((2, DEEP, HALF), jnp.bfloat16),
        "grads11": pltpu.VMEM((2, DEEP, HALF), jnp.bfloat16),
        "turned0": pltpu.VMEM((BLOCK_ROWS, 1024), jnp.bfloat16),
        "turned1": pltpu.VMEM((BLOCK_ROWS, 1024), jnp.bfloat16),
        "out": pltpu.VMEM((BUCKETS, 2, 2, 4, 16, HALF), F32),
        "rt": pltpu.VMEM((2, 4, 2, 1, 2048), F32),
        "rx": pltpu.VMEM((4, 2, 1, 2048), F32),
        "rxx": pltpu.VMEM((3, 2, 1, 2048), F32),
        "rxy": pltpu.VMEM((4, 1, 2048), F32),
        "rxz": pltpu.VMEM((4, 1, 2048), F32),
        "ry": pltpu.VMEM((2, 1, 2048), F32),
        "load_sem": pltpu.SemaphoreType.DMA((6,)),
        "state_sem": pltpu.SemaphoreType.DMA((3,)),
        "x_send": pltpu.SemaphoreType.DMA((SENT, 3)),
        "x_recv": pltpu.SemaphoreType.DMA((SENT, 3)),
        "p1_send": pltpu.SemaphoreType.DMA((RING, 3)),
        "p1_recv": pltpu.SemaphoreType.DMA((RING, 3, 2)),
        "p2_send": pltpu.SemaphoreType.DMA((RING, 3)),
        "p2_recv": pltpu.SemaphoreType.DMA((RING, 3, 2)),
        "p3_send": pltpu.SemaphoreType.DMA((RING, 3)),
        "p3_recv": pltpu.SemaphoreType.DMA((RING, 3)),
        "ag_send": pltpu.SemaphoreType.DMA((RING, 3)),
        "ag_recv": pltpu.SemaphoreType.DMA((RING, 5)),
        "d_recv": pltpu.SemaphoreType.DMA((3, 7)),
        "r_send": pltpu.SemaphoreType.DMA((4,)),
        "r_recv": pltpu.SemaphoreType.DMA((8,)),
    }
    for q in range(3):
        r = ROWS[q]
        tree[f"own{q}"] = pltpu.VMEM((OWN, 4, 4, 4, r, W), F32)
        tree[f"sent{q}"] = pltpu.VMEM((SENT, 4, 4, 4, r, W), F32)
        tree[f"xr{q}"] = pltpu.VMEM((4, 4, 4, 4, r, W), F32)
        tree[f"ra{q}"] = pltpu.VMEM((4, 6, 2, 4, r, W), F32)
        tree[f"q{q}"] = pltpu.VMEM((STEPS, 4, 4, r, W), F32)
        tree[f"rb{q}"] = pltpu.VMEM((STEPS, 12, r, W), F32)
        tree[f"rc{q}"] = pltpu.VMEM((STEPS, 3, r, W), F32)
    return tree


def kernel(names, order, logits, acts_hbm, keys_hbm, values_hbm, *refs):
    state_hbm, router_state = refs[0:3], refs[3:6]
    state, router_new = refs[6:9], refs[9:12]
    refs = refs[12:]
    ref = dict(zip(names, refs))
    rep = lax.axis_index("rep")
    inst = lax.axis_index("inst")
    yl, z = rep // 4, rep % 4
    yh, x, core = inst // 8, (inst // 2) % 4, inst % 2
    place = {"x": x, "y": yh * 2 + yl, "z": z, "c": core}

    def device(**change):
        at = {**place, **change}
        y = at["y"]
        return {"rep": (y % 2) * 4 + at["z"], "inst": ((y // 2) * 4 + at["x"]) * 2 + at["c"]}

    def along(dim, delta):
        return device(**{dim: (place[dim] + delta) % 4})

    sibling = device(c=1 - core)
    partner = device(y=yh * 2 + (1 - yl))

    def send(src, dst, send_sem, recv_sem, to):
        copy = pltpu.make_async_remote_copy(
            src_ref=src, dst_ref=dst, send_sem=send_sem, recv_sem=recv_sem, device_id=to, device_id_type=MESH
        )
        copy.start()

    def wait_recv(dst, sem):
        pltpu.make_async_copy(dst, dst, sem).wait()

    wait_send = wait_recv

    def grad_load(half, k):
        for n, part in enumerate((keys_hbm, values_hbm)):
            pltpu.make_async_copy(
                part.at[pl.ds(k * DEEP, DEEP), pl.ds(half * HALF, HALF)],
                ref[f"grads{half}{k}"].at[n],
                ref["load_sem"].at[2 + half * 2 + k],
            ).start()

    for k in range(2):
        grad_load(0, k)
        for i in range(16):
            pltpu.make_async_copy(
                acts_hbm.at[pl.ds(k * DEEP, DEEP), pl.ds(i * BLOCK_ROWS, BLOCK_ROWS)],
                ref[f"acts{k}"].at[i],
                ref["load_sem"].at[k],
            ).start()
    for k in range(2):
        grad_load(1, k)
    state_loads = [pltpu.make_async_copy(state_hbm[n], state[n], ref["state_sem"].at[n]) for n in range(3)]

    barrier = pltpu.get_barrier_semaphore()
    peers = [sibling] + [along(d, delta) for d in "xyz" for delta in (1, 2, 3)]
    for peer in peers:
        pl.semaphore_signal(barrier, inc=1, device_id=peer, device_id_type=MESH)

    def router_term():
        for i in range(16):
            block = jnp.concatenate([ref["acts0"][i], ref["acts1"][i]], axis=0)
            term = jnp.dot(logits[...], block, preferred_element_type=F32)
            for e in range(8):
                ref["rt"][i // 8, e % 4, e // 4, :, pl.ds((i % 8) * 256, 256)] = term[e : e + 1, :]

    def spots(q, slot_y, slot_x):
        pair, every = pl.ds(slot_y * 2, 2), pl.ds(0, 4)
        return ((slot_x, every, pair), (pair, slot_x, every), (every, pair, slot_x))[q]

    def exchange(step, j):
        for q in range(3):
            spot = spots(q, j // 4, j % 4)
            send(
                ref[f"sent{q}"].at[(step % SENT,) + spot],
                ref[f"xr{q}"].at[(step % 4,) + spot],
                ref["x_send"].at[step % SENT, q],
                ref["x_recv"].at[step % SENT, q],
                sibling,
            )

    def turn(step, j, into, halves):
        block = order[step // 2 * 8 + j] % 16
        for h, side in enumerate((core, 1 - core)):
            for k in halves:
                columns = ref[f"acts{k}"][block, :, pl.ds(pl.multiple_of(side * 128, 128), 128)]
                into[h * 128 : (h + 1) * 128, k * DEEP : (k + 1) * DEEP] = columns.T

    def matmul(step, first, last, halves=(0, 1)):
        bucket, par = step // 2, step % 2
        turn(step, first, ref["turned0"], halves)

        def body(pair, carry):
            j = first + pair * 2
            if 1 in halves:

                @pl.when(pair > 0)
                def _():
                    exchange(step, j - 1)

            dots(step, j, 0, j + 1)
            if 1 in halves:
                exchange(step, j)
            dots(step, j + 1, 1, jnp.minimum(j + 2, 7))
            return carry

        def dots(step, j, now, later):
            slot_y, slot_x = j // 4, j % 4
            block = order[bucket * 8 + j]
            turn(step, later, ref[f"turned{1 - now}"], halves)
            for n in range(2):
                lo = n * 256
                piece = jnp.dot(
                    ref[f"turned{now}"][:, halves[0] * DEEP : (halves[-1] + 1) * DEEP],
                    jnp.concatenate(
                        [ref[f"grads{par}{k}"][block // 16, :, lo : lo + 256] for k in halves], axis=0
                    ),
                    preferred_element_type=F32,
                )
                for h in range(2):
                    dst = "sent" if h else "own"
                    slot = step % (SENT if h else OWN)
                    for q in range(3):
                        for chunk, top, count, row in PARTS[q]:
                            if chunk // 2 != n:
                                continue
                            left = chunk % 2 * W
                            for l in range(2):
                                y = slot_y * 2 + l
                                for k in range(4):
                                    start = h * 128 + l * 64 + k * 16 + top
                                    value = piece[start : start + count, left : left + W]
                                    at = ((slot_x, k, y), (y, slot_x, k), (k, y, slot_x))[q]
                                    spot = (slot,) + at + (pl.ds(row, count),)
                                    if halves == (1,):
                                        value = ref[f"{dst}{q}"][spot] + value
                                    ref[f"{dst}{q}"][spot] = value

        lax.fori_loop(0, (last - first) // 2, body, 0)
        if 1 in halves:
            exchange(step, last - 1)

    def add_sibling(step):
        for q in range(3):
            own, xr = ref[f"own{q}"], ref[f"xr{q}"]
            wait_recv(xr.at[step % 4], ref["x_recv"].at[step % SENT, q])

            def body(d, carry):
                own[step % OWN, d] = own[step % OWN, d] + xr[step % 4, d]
                return carry

            lax.fori_loop(0, 4, body, 0)

    def views(step, q, phase):
        slot = step % OWN if phase == 1 else step
        src, recv = (ref[f"own{q}"], ref[f"ra{q}"]) if phase == 1 else (ref[f"q{q}"], ref[f"rb{q}"])
        at = lambda d, h: (slot, d, pl.ds(2 * h, 2))
        into = (lambda m: (step % 4, m)) if phase == 1 else (lambda m: (step, pl.ds(2 * m, 2)))
        return src, at, recv, into

    def group(step, phase, first, count):
        return (step % 4, pl.ds(first, count)) if phase == 1 else (step, pl.ds(2 * first, 2 * count))

    def ring_send(step, q, phase, m, where, delta):
        src, at, recv, into = views(step, q, phase)
        dim = DIMS[q][phase - 1]
        d, h = where
        send(
            src.at[at((place[dim] + d) % 4, h)],
            recv.at[into(m)],
            ref[f"p{phase}_send"].at[step % RING, q],
            ref[f"p{phase}_recv"].at[step % RING, q, int(m > 1)],
            along(dim, delta),
        )

    def ring_start(step, phase):
        for q in range(3):
            ring_send(step, q, phase, 0, (2, 0), 1)
            ring_send(step, q, phase, 1, (2, 1), 3)

    def ring_next(step, phase):
        for q in range(3):
            ring_send(step, q, phase, 2, (1, 1), 1)
            ring_send(step, q, phase, 3, (3, 0), 3)

    def ring_relay(step, phase):
        for q in range(3):
            src, at, recv, into = views(step, q, phase)
            here = place[DIMS[q][phase - 1]]
            wait_recv(recv.at[group(step, phase, 0, 2)], ref[f"p{phase}_recv"].at[step % RING, q, 0])
            for m, d, h in ((0, 1, 0), (1, 3, 1)):
                spot = at((here + d) % 4, h)
                src[spot] = src[spot] + recv[into(m)]
                ring_send(step, q, phase, 4 + m, (d, h), d)

    def ring_end(step, phase):
        for q in range(3):
            src, at, recv, into = views(step, q, phase)
            here = place[DIMS[q][phase - 1]]
            wait_recv(recv.at[group(step, phase, 2, 4)], ref[f"p{phase}_recv"].at[step % RING, q, 1])
            for h, arrived in ((0, (3, 4)), (1, (2, 5))):
                spot = at(here, h)
                total = src[spot] + recv[into(arrived[0])] + recv[into(arrived[1])]
                if phase == 1:
                    ref[f"q{q}"][step, pl.ds(2 * h, 2)] = total
                else:
                    src[spot] = total

    def ring_sent(step, phase):
        for q in range(3):
            recv = views(step, q, phase)[2]
            wait_send(recv.at[group(step, phase, 0, 6)], ref[f"p{phase}_send"].at[step % RING, q])

    def second_start(step):
        for m, delta in enumerate((2, 1, 3)):
            for q in range(3):
                dim = DIMS[q][1]
                send(
                    ref[f"q{q}"].at[step, (place[dim] + delta) % 4],
                    ref[f"rb{q}"].at[step, pl.ds(4 * m, 4)],
                    ref["p2_send"].at[step % RING, q],
                    ref["p2_recv"].at[step % RING, q, 0],
                    along(dim, delta),
                )

    def second_end(step):
        for q in range(3):
            rb, here = ref[f"rb{q}"], place[DIMS[q][1]]
            wait_recv(rb.at[step], ref["p2_recv"].at[step % RING, q, 0])
            total = ref[f"q{q}"][step, here]
            for m in range(3):
                total = total + rb[step, pl.ds(4 * m, 4)]
            ref[f"q{q}"][step, here] = total

    def exchange_sent(step):
        for q in range(3):
            wait_send(ref[f"xr{q}"].at[step % 4], ref["x_send"].at[step % SENT, q])

    def last_start(step):
        for q in range(3):
            second, third = DIMS[q][1:]
            for m in range(3):
                delta = (1, 3, 2)[m]
                send(
                    ref[f"q{q}"].at[step, place[second], (place[third] + delta) % 4],
                    ref[f"rc{q}"].at[step, m],
                    ref["p3_send"].at[step % RING, q],
                    ref["p3_recv"].at[step % RING, q],
                    along(third, delta),
                )

    def last_end(step):
        b, par = step // 2, step % 2
        for q in range(3):
            second, third = DIMS[q][1:]
            rc = ref[f"rc{q}"]
            wait_recv(rc.at[step], ref["p3_recv"].at[step % RING, q])
            total = ref[f"q{q}"][step, place[second], place[third]] + rc[step, 0] + rc[step, 1] + rc[step, 2]
            for chunk, top, count, row in PARTS[q]:
                ref["out"][b, par, yl, z, pl.ds(top, count), pl.ds(chunk * W, W)] = total[row : row + count]

    def last_sent(step):
        for q in range(3):
            wait_send(ref[f"rc{q}"].at[step], ref["p3_send"].at[step % RING, q])

    def gather_send(step, n, spot, to):
        out = ref["out"].at[(step // 2, step % 2) + spot]
        send(out, out, ref["ag_send"].at[step % RING, (n + 1) // 2], ref["ag_recv"].at[step % RING, n], to)

    def gather_wait(step, n, spot):
        wait_recv(ref["out"].at[(step // 2, step % 2) + spot], ref["ag_recv"].at[step % RING, n])

    both = pl.ds(0, 2)

    def gather_partner(step):
        gather_send(step, 0, (yl, z), partner)

    def gather_start(step):
        gather_wait(step, 0, (1 - yl, z))
        gather_send(step, 1, (both, z), along("z", 1))
        gather_send(step, 2, (both, z), along("z", 3))

    def gather_relay(step):
        gather_wait(step, 1, (both, (z + 3) % 4))
        gather_send(step, 3, (0, (z + 3) % 4), along("z", 1))
        gather_wait(step, 2, (both, (z + 1) % 4))
        gather_send(step, 4, (1, (z + 1) % 4), along("z", 3))

    def gather_direct(step):
        b, par = step // 2, step % 2
        own = ref["out"].at[b, par, yl, z]
        for count, n in enumerate((5, 1, 6, 2, 4, 0, 3)):
            dy, dz = divmod(n + 1, 4)
            to = device(y=yh * 2 + (yl + dy) % 2, z=(z + dz) % 4)
            sent = (0, 1, 1, 1, 1, 2, 2)[count]
            send(own, own, ref["ag_send"].at[step % RING, sent], ref["d_recv"].at[STEPS - 1 - step, n], to)

    def gather_end(step):
        if step in DIRECT_GATHER:
            for n in range(7):
                dy, dz = divmod(n + 1, 4)
                there = ref["out"].at[step // 2, step % 2, (yl + dy) % 2, (z - dz) % 4]
                wait_recv(there, ref["d_recv"].at[STEPS - 1 - step, n])
        else:
            gather_wait(step, 3, (0, (z + 2) % 4))
            gather_wait(step, 4, (1, (z + 2) % 4))
        b, par = step // 2, step % 2
        columns = pl.ds(par * HALF, HALF)

        def body(i, carry):
            rows = pl.ds(pl.multiple_of(i * 16, 16), 16)
            grad = ref["out"][b, par, i // 4, i % 4]
            fresh = adamw(grad, *(part[b, rows, columns] for part in state))
            for part, value in zip(state, fresh):
                part[b, rows, columns] = value
            return carry

        lax.fori_loop(0, 8, body, 0)

    def gather_sent(step):
        out = ref["out"].at[step // 2, step % 2]
        for n, part in enumerate((out.at[0, 0], out.at[0], out.at[both, 0])):
            wait_send(part, ref["ag_send"].at[step % RING, n])

    def state_start():
        for load in state_loads:
            load.start()

    def state_end():
        for load in state_loads:
            load.wait()

    def router_send(n, src, dst, to):
        send(src, dst, ref["r_send"].at[(n + 2) // 3], ref["r_recv"].at[max(n - 2, min(n, 1))], to)

    def router_wait(n, dst):
        wait_recv(dst, ref["r_recv"].at[max(n - 2, min(n, 1))])

    def router_0():
        router_send(0, ref["rt"].at[1 - core], ref["rx"], sibling)

    def router_1():
        router_wait(0, ref["rx"])
        ref["rt"][core] = ref["rt"][core] + ref["rx"][...]
        for m, delta in enumerate((1, 2, 3)):
            router_send(1 + m, ref["rt"].at[core, (x + delta) % 4], ref["rxx"].at[m], along("x", delta))

    def router_2():
        router_wait(1, ref["rxx"])
        ref["ry"][...] = ref["rt"][core, x] + ref["rxx"][0] + ref["rxx"][1] + ref["rxx"][2]
        here = place["y"]
        ref["rxy"][here] = ref["ry"][yh]
        for m, delta in enumerate((1, 2, 3)):
            to = (here + delta) % 4
            router_send(4 + m, ref["ry"].at[to // 2], ref["rxy"].at[here], along("y", delta))

    def router_3():
        here = place["y"]
        for m, delta in enumerate((1, 2, 3)):
            router_wait(4 + m, ref["rxy"].at[(here - delta) % 4])
        total = ref["rxy"][0] + ref["rxy"][1] + ref["rxy"][2] + ref["rxy"][3]
        ref["rxz"][z] = total
        for m, delta in enumerate((1, 2, 3)):
            router_send(7 + m, ref["rxz"].at[z], ref["rxz"].at[z], along("z", delta))

    def router_4():
        for m, delta in enumerate((1, 2, 3)):
            router_wait(7 + m, ref["rxz"].at[(z - delta) % 4])
        total = ref["rxz"][0] + ref["rxz"][1] + ref["rxz"][2] + ref["rxz"][3]
        for row in range(2):
            at = pl.ds(row, 1)
            fresh = adamw(total[:, row * 1024 : (row + 1) * 1024], *(part[at] for part in router_state))
            for part, value in zip(router_new, fresh):
                part[at] = value

    def router_sent():
        wait_send(ref["rx"], ref["r_send"].at[0])
        wait_send(ref["rxx"], ref["r_send"].at[1])
        wait_send(ref["rxy"].at[pl.ds(0, 3)], ref["r_send"].at[2])
        wait_send(ref["rxz"].at[pl.ds(0, 3)], ref["r_send"].at[3])

    router_stages = {0: router_0, 1: router_1, 2: router_2, 3: router_3, 4: router_4}

    def run(stage, *args):
        with jax.named_scope(f"{stage.__name__}#s={'_'.join(map(str, args)).replace(' ', '')}"):
            stage(*args)

    def live(step):
        return 0 <= step < STEPS

    def loaded(k):
        wait_recv(ref[f"grads0{k}"], ref["load_sem"].at[2 + k])
        wait_recv(ref[f"acts{k}"], ref["load_sem"].at[k])

    run(loaded, 0)
    run(matmul, 0, 0, 8, (0,))
    run(loaded, 1)
    with jax.named_scope("barrier"):
        pl.semaphore_wait(barrier, len(peers))
    run(matmul, 0, 0, 8, (1,))
    run(add_sibling, 0)
    run(ring_start, 0, 1)

    def second(step):
        run(ring_end, step, 1)
        if step in DIRECT:
            run(second_start, step)
        else:
            run(ring_start, step, 2)
            run(ring_next, step, 2)

    def third(step):
        if step in DIRECT:
            run(second_end, step)
        else:
            run(ring_end, step, 2)
        run(last_start, step)

    def spread(step):
        run(last_end, step)
        ring_sent(step, 2)
        last_sent(step)
        if step in DIRECT_GATHER:
            run(gather_direct, step)
        else:
            run(gather_partner, step)

    def finish(step):
        run(gather_end, step)
        run(gather_sent, step)

    for i in range(STEPS):
        if live(i - 2):
            run(ring_relay, i - 2, 2)
        run(ring_next, i, 1)
        if i == 0:
            run(router_term)
            run(router_0)
            for k in range(2):
                wait_recv(ref[f"grads1{k}"], ref["load_sem"].at[4 + k])
            state_start()
        if live(i + 1):
            if live(i - 1):
                run(exchange_sent, i - 1)
            if live(i - 3):
                run(ring_sent, i - 3, 1)
            run(matmul, i + 1, 0, 4)
        if live(i - 1):
            second(i - 1)
        if live(i - 3):
            spread(i - 3)
        if live(i - 4):
            run(gather_start, i - 4)
        if live(i + 1):
            run(matmul, i + 1, 4, 8)
        run(ring_relay, i, 1)
        if live(i - 2):
            third(i - 2)
        if live(i + 1):
            run(add_sibling, i + 1)
            run(ring_start, i + 1, 1)
        if live(i - 4) and i < STEPS - 1:
            run(gather_relay, i - 4)
        if i + 1 in router_stages:
            run(router_stages[i + 1])
        if live(i - 5) and i < STEPS - 1:
            if i == 5:
                run(state_end)
            finish(i - 5)
    last = STEPS - 1
    run(ring_relay, last - 1, 2)
    run(gather_relay, last - 4)
    run(gather_start, last - 3)
    second(last)
    third(last - 1)
    spread(last - 2)
    run(gather_relay, last - 3)
    finish(last - 5)
    third(last)
    run(gather_start, last - 2)
    spread(last - 1)
    finish(last - 4)
    spread(last)
    run(gather_relay, last - 2)
    for step in range(last - 3, last + 1):
        finish(step)
    with jax.named_scope("ending"):
        for step in range(STEPS - 4, STEPS):
            if step >= STEPS - 2:
                exchange_sent(step)
            ring_sent(step, 1)
        router_sent()


def on_device(
    acts,
    grad_keys,
    grad_values,
    grad_logits,
    order,
    bucket_param,
    bucket_m,
    bucket_v,
    router_param,
    router_m,
    router_v,
):
    tree = scratch()
    names = tuple(tree)
    hbm, vmem = pl.BlockSpec(memory_space=pltpu.HBM), pl.BlockSpec(memory_space=pltpu.VMEM)
    fresh = pl.pallas_call(
        lambda *refs: kernel(names, *refs),
        out_shape=tuple(
            pltpu.VMEM(part.shape, F32) for part in (bucket_param, bucket_m, bucket_v, router_param, router_m, router_v)
        ),
        in_specs=[pl.BlockSpec(memory_space=pltpu.SMEM), vmem] + [hbm] * 6 + [vmem] * 3,
        out_specs=(vmem,) * 6,
        scratch_shapes=list(tree.values()),
        compiler_params=pltpu.CompilerParams(
            collective_id=0, has_side_effects=True, vmem_limit_bytes=VMEM_LIMIT
        ),
        cost_estimate=pl.CostEstimate(flops=17_200_000_000, bytes_accessed=24_000_000, transcendentals=0),
        name="reduce",
    )(
        order,
        grad_logits,
        acts,
        grad_keys,
        grad_values,
        bucket_param,
        bucket_m,
        bucket_v,
        router_param,
        router_m,
        router_v,
    )
    return pl.pallas_call(
        store,
        out_shape=tuple(jax.ShapeDtypeStruct(part.shape, F32) for part in fresh),
        in_specs=[vmem] * 6,
        out_specs=(hbm,) * 6,
        scratch_shapes=[pltpu.SemaphoreType.DMA((15,))],
        compiler_params=pltpu.CompilerParams(vmem_limit_bytes=1024 * 1024),
        name="store",
    )(*(pltpu.with_memory_space_constraint(part, pltpu.VMEM) for part in fresh))


def store(*refs):
    copies = []
    for n in range(3):
        copies.append((refs[3 + n], refs[9 + n]))
        for b in range(BUCKETS):
            copies.append((refs[n].at[b], refs[6 + n].at[b]))
    copies = [pltpu.make_async_copy(src, dst, refs[12].at[n]) for n, (src, dst) in enumerate(copies)]
    for copy in copies:
        copy.start()
    for copy in copies:
        copy.wait()


def solution(mesh):
    state, router = P(None, "inst", None), P("inst", None)
    tokens = P(("rep", "inst"), None)
    return jax.shard_map(
        on_device,
        mesh=mesh,
        in_specs=(tokens, tokens, tokens, P(None, ("rep", "inst")), P(), state, state, state, router, router, router),
        out_specs=(state, state, state, router, router, router),
        check_vma=False,
    )
```

```python
import jax
import jax.numpy as jnp
from jax import lax
from jax.experimental import pallas as pl
from jax.experimental.pallas import tpu as pltpu
from jax.sharding import PartitionSpec as P

BUCKETS = 4
BLOCK_ROWS = 256
STEPS = 8
HALF = 512
DEEP = 512

beta_first = 0.9
beta_second = 0.95
step_rate = 0.05
decay_rate = 0.1
epsilon = 1e-08
correct_first = 1.0 - 0.9**10
correct_second = 1.0 - 0.95**10

VMEM_LIMIT = 56 * 1024 * 1024
MESH = pl.DeviceIdType.MESH
F32 = jnp.float32

DIMS = (("x", "z", "y"), ("y", "x", "z"), ("z", "y", "x"))
PARTS = (((0, 0, 16, 0), (3, 0, 8, 16)), ((1, 0, 16, 0), (3, 8, 8, 16)), ((2, 0, 16, 0),))
ROWS = (24, 24, 16)
W = 128
OWN = 4
SENT = 2
RING = 4
DIRECT = (STEPS - 1,)
DIRECT_GATHER = (STEPS - 2, STEPS - 1)


def adamw(grad, param, moment, second):
    moment_new = beta_first * moment + (1.0 - beta_first) * grad
    second_new = beta_second * second + (1.0 - beta_second) * grad * grad
    ratio = moment_new / correct_first / (jnp.sqrt(second_new / correct_second) + epsilon)
    param_new = param - step_rate * (ratio + decay_rate * param)
    return (param_new, moment_new, second_new)


def scratch():
    tree = {
        "acts0": pltpu.VMEM((16, DEEP, BLOCK_ROWS), jnp.bfloat16),
        "acts1": pltpu.VMEM((16, DEEP, BLOCK_ROWS), jnp.bfloat16),
        "grads00": pltpu.VMEM((2, DEEP, HALF), jnp.bfloat16),
        "grads01": pltpu.VMEM((2, DEEP, HALF), jnp.bfloat16),
        "grads10": pltpu.VMEM((2, DEEP, HALF), jnp.bfloat16),
        "grads11": pltpu.VMEM((2, DEEP, HALF), jnp.bfloat16),
        "turned0": pltpu.VMEM((BLOCK_ROWS, 1024), jnp.bfloat16),
        "turned1": pltpu.VMEM((BLOCK_ROWS, 1024), jnp.bfloat16),
        "out": pltpu.VMEM((BUCKETS, 2, 2, 4, 16, HALF), F32),
        "rt": pltpu.VMEM((2, 4, 2, 1, 2048), F32),
        "rx": pltpu.VMEM((4, 2, 1, 2048), F32),
        "rxx": pltpu.VMEM((3, 2, 1, 2048), F32),
        "rxy": pltpu.VMEM((4, 1, 2048), F32),
        "rxz": pltpu.VMEM((4, 1, 2048), F32),
        "ry": pltpu.VMEM((2, 1, 2048), F32),
        "load_sem": pltpu.SemaphoreType.DMA((6,)),
        "state_sem": pltpu.SemaphoreType.DMA((3,)),
        "order": pltpu.SMEM((32,), jnp.int32),
        "logits": pltpu.VMEM((8, 1024), jnp.bfloat16),
        "router": pltpu.VMEM((3, 2, 1024), F32),
        "small_sem": pltpu.SemaphoreType.DMA((5,)),
        "x_send": pltpu.SemaphoreType.DMA((SENT, 3)),
        "x_recv": pltpu.SemaphoreType.DMA((SENT, 3)),
        "p1_send": pltpu.SemaphoreType.DMA((RING, 3)),
        "p1_recv": pltpu.SemaphoreType.DMA((RING, 3, 2)),
        "p2_send": pltpu.SemaphoreType.DMA((RING, 3)),
        "p2_recv": pltpu.SemaphoreType.DMA((RING, 3, 2)),
        "p3_send": pltpu.SemaphoreType.DMA((RING, 3)),
        "p3_recv": pltpu.SemaphoreType.DMA((RING, 3)),
        "ag_send": pltpu.SemaphoreType.DMA((RING, 3)),
        "ag_recv": pltpu.SemaphoreType.DMA((RING, 5)),
        "d_recv": pltpu.SemaphoreType.DMA((2, 7)),
        "r_send": pltpu.SemaphoreType.DMA((4,)),
        "r_recv": pltpu.SemaphoreType.DMA((8,)),
    }
    for q in range(3):
        r = ROWS[q]
        tree[f"own{q}"] = pltpu.VMEM((OWN, 4, 4, 4, r, W), F32)
        tree[f"sent{q}"] = pltpu.VMEM((SENT, 4, 4, 4, r, W), F32)
        tree[f"xr{q}"] = pltpu.VMEM((4, 4, 4, 4, r, W), F32)
        tree[f"ra{q}"] = pltpu.VMEM((4, 6, 2, 4, r, W), F32)
        tree[f"q{q}"] = pltpu.VMEM((STEPS, 4, 4, r, W), F32)
        tree[f"rb{q}"] = pltpu.VMEM((STEPS, 12, r, W), F32)
        tree[f"rc{q}"] = pltpu.VMEM((STEPS, 3, r, W), F32)
    return tree


def kernel(names, order_hbm, logits_hbm, acts_hbm, keys_hbm, values_hbm, *refs):
    state_hbm, router_hbm = refs[0:3], refs[3:6]
    state, router_new = refs[6:9], refs[9:12]
    refs = refs[12:]
    ref = dict(zip(names, refs))
    rep = lax.axis_index("rep")
    inst = lax.axis_index("inst")
    yl, z = rep // 4, rep % 4
    yh, x, core = inst // 8, (inst // 2) % 4, inst % 2
    place = {"x": x, "y": yh * 2 + yl, "z": z, "c": core}

    def device(**change):
        at = {**place, **change}
        y = at["y"]
        return {"rep": (y % 2) * 4 + at["z"], "inst": ((y // 2) * 4 + at["x"]) * 2 + at["c"]}

    def along(dim, delta):
        return device(**{dim: (place[dim] + delta) % 4})

    sibling = device(c=1 - core)
    partner = device(y=yh * 2 + (1 - yl))

    def send(src, dst, send_sem, recv_sem, to):
        copy = pltpu.make_async_remote_copy(
            src_ref=src, dst_ref=dst, send_sem=send_sem, recv_sem=recv_sem, device_id=to, device_id_type=MESH
        )
        copy.start()

    def wait_recv(dst, sem):
        pltpu.make_async_copy(dst, dst, sem).wait()

    wait_send = wait_recv

    def grad_load(half, k):
        for n, part in enumerate((keys_hbm, values_hbm)):
            pltpu.make_async_copy(
                part.at[pl.ds(k * DEEP, DEEP), pl.ds(half * HALF, HALF)],
                ref[f"grads{half}{k}"].at[n],
                ref["load_sem"].at[2 + half * 2 + k],
            ).start()

    order, logits = ref["order"], ref["logits"]
    router_state = [ref["router"].at[n] for n in range(3)]
    small = [(order_hbm, order), (logits_hbm, logits)] + list(zip(router_hbm, router_state))
    small = [pltpu.make_async_copy(src, dst, ref["small_sem"].at[n]) for n, (src, dst) in enumerate(small)]
    for copy in small:
        copy.start()
    for k in range(2):
        grad_load(0, k)
        for i in range(16):
            pltpu.make_async_copy(
                acts_hbm.at[pl.ds(k * DEEP, DEEP), pl.ds(i * BLOCK_ROWS, BLOCK_ROWS)],
                ref[f"acts{k}"].at[i],
                ref["load_sem"].at[k],
            ).start()
    for k in range(2):
        grad_load(1, k)
    state_loads = [pltpu.make_async_copy(state_hbm[n], state[n], ref["state_sem"].at[n]) for n in range(3)]

    barrier = pltpu.get_barrier_semaphore()
    peers = [sibling] + [along(d, delta) for d in "xyz" for delta in (1, 2, 3)]
    for peer in peers:
        pl.semaphore_signal(barrier, inc=1, device_id=peer, device_id_type=MESH)

    def router_term():
        for i in range(16):
            block = jnp.concatenate([ref["acts0"][i], ref["acts1"][i]], axis=0)
            term = jnp.dot(logits[...], block, preferred_element_type=F32)
            for e in range(8):
                ref["rt"][i // 8, e % 4, e // 4, :, pl.ds((i % 8) * 256, 256)] = term[e : e + 1, :]

    def spots(q, slot_y, slot_x):
        pair, every = pl.ds(slot_y * 2, 2), pl.ds(0, 4)
        return ((slot_x, every, pair), (pair, slot_x, every), (every, pair, slot_x))[q]

    def exchange(step, j):
        for q in range(3):
            spot = spots(q, j // 4, j % 4)
            send(
                ref[f"sent{q}"].at[(step % SENT,) + spot],
                ref[f"xr{q}"].at[(step % 4,) + spot],
                ref["x_send"].at[step % SENT, q],
                ref["x_recv"].at[step % SENT, q],
                sibling,
            )

    def turn(step, j, into, halves):
        block = order[step // 2 * 8 + j] % 16
        for h, side in enumerate((core, 1 - core)):
            for k in halves:
                columns = ref[f"acts{k}"][block, :, pl.ds(pl.multiple_of(side * 128, 128), 128)]
                into[h * 128 : (h + 1) * 128, k * DEEP : (k + 1) * DEEP] = columns.T

    def matmul(step, first, last, halves=(0, 1)):
        bucket, par = step // 2, step % 2
        turn(step, first, ref["turned0"], halves)

        def body(pair, carry):
            j = first + pair * 2
            if 1 in halves:

                @pl.when(pair > 0)
                def _():
                    exchange(step, j - 1)

            dots(step, j, 0, j + 1)
            if 1 in halves:
                exchange(step, j)
            dots(step, j + 1, 1, jnp.minimum(j + 2, 7))
            return carry

        def dots(step, j, now, later):
            slot_y, slot_x = j // 4, j % 4
            block = order[bucket * 8 + j]
            turn(step, later, ref[f"turned{1 - now}"], halves)
            for n in range(2):
                lo = n * 256
                piece = jnp.dot(
                    ref[f"turned{now}"][:, halves[0] * DEEP : (halves[-1] + 1) * DEEP],
                    jnp.concatenate(
                        [ref[f"grads{par}{k}"][block // 16, :, lo : lo + 256] for k in halves], axis=0
                    ),
                    preferred_element_type=F32,
                )
                for h in range(2):
                    dst = "sent" if h else "own"
                    slot = step % (SENT if h else OWN)
                    for q in range(3):
                        for chunk, top, count, row in PARTS[q]:
                            if chunk // 2 != n:
                                continue
                            left = chunk % 2 * W
                            for l in range(2):
                                y = slot_y * 2 + l
                                for k in range(4):
                                    start = h * 128 + l * 64 + k * 16 + top
                                    value = piece[start : start + count, left : left + W]
                                    at = ((slot_x, k, y), (y, slot_x, k), (k, y, slot_x))[q]
                                    spot = (slot,) + at + (pl.ds(row, count),)
                                    if halves == (1,):
                                        value = ref[f"{dst}{q}"][spot] + value
                                    ref[f"{dst}{q}"][spot] = value

        lax.fori_loop(0, (last - first) // 2, body, 0)
        if 1 in halves:
            exchange(step, last - 1)

    def add_sibling(step):
        for q in range(3):
            own, xr = ref[f"own{q}"], ref[f"xr{q}"]
            wait_recv(xr.at[step % 4], ref["x_recv"].at[step % SENT, q])

            def body(d, carry):
                own[step % OWN, d] = own[step % OWN, d] + xr[step % 4, d]
                return carry

            lax.fori_loop(0, 4, body, 0)

    def views(step, q, phase):
        slot = step % OWN if phase == 1 else step
        src, recv = (ref[f"own{q}"], ref[f"ra{q}"]) if phase == 1 else (ref[f"q{q}"], ref[f"rb{q}"])
        at = lambda d, h: (slot, d, pl.ds(2 * h, 2))
        into = (lambda m: (step % 4, m)) if phase == 1 else (lambda m: (step, pl.ds(2 * m, 2)))
        return src, at, recv, into

    def group(step, phase, first, count):
        return (step % 4, pl.ds(first, count)) if phase == 1 else (step, pl.ds(2 * first, 2 * count))

    def ring_send(step, q, phase, m, where, delta):
        src, at, recv, into = views(step, q, phase)
        dim = DIMS[q][phase - 1]
        d, h = where
        send(
            src.at[at((place[dim] + d) % 4, h)],
            recv.at[into(m)],
            ref[f"p{phase}_send"].at[step % RING, q],
            ref[f"p{phase}_recv"].at[step % RING, q, int(m > 1)],
            along(dim, delta),
        )

    def ring_start(step, phase):
        for q in range(3):
            ring_send(step, q, phase, 0, (2, 0), 1)
            ring_send(step, q, phase, 1, (2, 1), 3)

    def ring_next(step, phase):
        for q in range(3):
            ring_send(step, q, phase, 2, (1, 1), 1)
            ring_send(step, q, phase, 3, (3, 0), 3)

    def ring_relay(step, phase):
        for q in range(3):
            src, at, recv, into = views(step, q, phase)
            here = place[DIMS[q][phase - 1]]
            wait_recv(recv.at[group(step, phase, 0, 2)], ref[f"p{phase}_recv"].at[step % RING, q, 0])
            for m, d, h in ((0, 1, 0), (1, 3, 1)):
                spot = at((here + d) % 4, h)
                src[spot] = src[spot] + recv[into(m)]
                ring_send(step, q, phase, 4 + m, (d, h), d)

    def ring_end(step, phase):
        for q in range(3):
            src, at, recv, into = views(step, q, phase)
            here = place[DIMS[q][phase - 1]]
            wait_recv(recv.at[group(step, phase, 2, 4)], ref[f"p{phase}_recv"].at[step % RING, q, 1])
            for h, arrived in ((0, (3, 4)), (1, (2, 5))):
                spot = at(here, h)
                total = src[spot] + recv[into(arrived[0])] + recv[into(arrived[1])]
                if phase == 1:
                    ref[f"q{q}"][step, pl.ds(2 * h, 2)] = total
                else:
                    src[spot] = total

    def ring_sent(step, phase):
        for q in range(3):
            recv = views(step, q, phase)[2]
            wait_send(recv.at[group(step, phase, 0, 6)], ref[f"p{phase}_send"].at[step % RING, q])

    def second_start(step):
        for m, delta in enumerate((2, 1, 3)):
            for q in range(3):
                dim = DIMS[q][1]
                send(
                    ref[f"q{q}"].at[step, (place[dim] + delta) % 4],
                    ref[f"rb{q}"].at[step, pl.ds(4 * m, 4)],
                    ref["p2_send"].at[step % RING, q],
                    ref["p2_recv"].at[step % RING, q, 0],
                    along(dim, delta),
                )

    def second_end(step):
        for q in range(3):
            rb, here = ref[f"rb{q}"], place[DIMS[q][1]]
            wait_recv(rb.at[step], ref["p2_recv"].at[step % RING, q, 0])
            total = ref[f"q{q}"][step, here]
            for m in range(3):
                total = total + rb[step, pl.ds(4 * m, 4)]
            ref[f"q{q}"][step, here] = total

    def exchange_sent(step):
        for q in range(3):
            wait_send(ref[f"xr{q}"].at[step % 4], ref["x_send"].at[step % SENT, q])

    def last_start(step):
        for q in range(3):
            second, third = DIMS[q][1:]
            for m in range(3):
                delta = (1, 3, 2)[m]
                send(
                    ref[f"q{q}"].at[step, place[second], (place[third] + delta) % 4],
                    ref[f"rc{q}"].at[step, m],
                    ref["p3_send"].at[step % RING, q],
                    ref["p3_recv"].at[step % RING, q],
                    along(third, delta),
                )

    def last_end(step):
        b, par = step // 2, step % 2
        for q in range(3):
            second, third = DIMS[q][1:]
            rc = ref[f"rc{q}"]
            wait_recv(rc.at[step], ref["p3_recv"].at[step % RING, q])
            total = ref[f"q{q}"][step, place[second], place[third]] + rc[step, 0] + rc[step, 1] + rc[step, 2]
            for chunk, top, count, row in PARTS[q]:
                ref["out"][b, par, yl, z, pl.ds(top, count), pl.ds(chunk * W, W)] = total[row : row + count]

    def last_sent(step):
        for q in range(3):
            wait_send(ref[f"rc{q}"].at[step], ref["p3_send"].at[step % RING, q])

    def gather_send(step, n, spot, to):
        out = ref["out"].at[(step // 2, step % 2) + spot]
        send(out, out, ref["ag_send"].at[step % RING, (n + 1) // 2], ref["ag_recv"].at[step % RING, n], to)

    def gather_wait(step, n, spot):
        wait_recv(ref["out"].at[(step // 2, step % 2) + spot], ref["ag_recv"].at[step % RING, n])

    both = pl.ds(0, 2)

    def gather_partner(step):
        gather_send(step, 0, (yl, z), partner)

    def gather_start(step):
        gather_wait(step, 0, (1 - yl, z))
        gather_send(step, 1, (both, z), along("z", 1))
        gather_send(step, 2, (both, z), along("z", 3))

    def gather_relay(step):
        gather_wait(step, 1, (both, (z + 3) % 4))
        gather_send(step, 3, (0, (z + 3) % 4), along("z", 1))
        gather_wait(step, 2, (both, (z + 1) % 4))
        gather_send(step, 4, (1, (z + 1) % 4), along("z", 3))

    def gather_direct(step):
        b, par = step // 2, step % 2
        own = ref["out"].at[b, par, yl, z]
        for count, n in enumerate((5, 1, 6, 2, 4, 0, 3)):
            dy, dz = divmod(n + 1, 4)
            to = device(y=yh * 2 + (yl + dy) % 2, z=(z + dz) % 4)
            sent = (0, 1, 1, 1, 1, 2, 2)[count]
            send(own, own, ref["ag_send"].at[step % RING, sent], ref["d_recv"].at[STEPS - 1 - step, n], to)

    def gather_end(step):
        if step in DIRECT_GATHER:
            for n in range(7):
                dy, dz = divmod(n + 1, 4)
                there = ref["out"].at[step // 2, step % 2, (yl + dy) % 2, (z - dz) % 4]
                wait_recv(there, ref["d_recv"].at[STEPS - 1 - step, n])
        else:
            gather_wait(step, 3, (0, (z + 2) % 4))
            gather_wait(step, 4, (1, (z + 2) % 4))
        b, par = step // 2, step % 2
        columns = pl.ds(par * HALF, HALF)

        def body(i, carry):
            rows = pl.ds(pl.multiple_of(i * 16, 16), 16)
            grad = ref["out"][b, par, i // 4, i % 4]
            fresh = adamw(grad, *(part[b, rows, columns] for part in state))
            for part, value in zip(state, fresh):
                part[b, rows, columns] = value
            return carry

        lax.fori_loop(0, 8, body, 0)

    def gather_sent(step):
        out = ref["out"].at[step // 2, step % 2]
        for n, part in enumerate((out.at[0, 0], out.at[0], out.at[both, 0])):
            wait_send(part, ref["ag_send"].at[step % RING, n])

    def state_start():
        for load in state_loads:
            load.start()

    def state_end():
        for load in state_loads:
            load.wait()

    def router_send(n, src, dst, to):
        send(src, dst, ref["r_send"].at[(n + 2) // 3], ref["r_recv"].at[max(n - 2, min(n, 1))], to)

    def router_wait(n, dst):
        wait_recv(dst, ref["r_recv"].at[max(n - 2, min(n, 1))])

    def router_0():
        router_send(0, ref["rt"].at[1 - core], ref["rx"], sibling)

    def router_1():
        router_wait(0, ref["rx"])
        ref["rt"][core] = ref["rt"][core] + ref["rx"][...]
        for m, delta in enumerate((1, 2, 3)):
            router_send(1 + m, ref["rt"].at[core, (x + delta) % 4], ref["rxx"].at[m], along("x", delta))

    def router_2():
        router_wait(1, ref["rxx"])
        ref["ry"][...] = ref["rt"][core, x] + ref["rxx"][0] + ref["rxx"][1] + ref["rxx"][2]
        here = place["y"]
        ref["rxy"][here] = ref["ry"][yh]
        for m, delta in enumerate((1, 2, 3)):
            to = (here + delta) % 4
            router_send(4 + m, ref["ry"].at[to // 2], ref["rxy"].at[here], along("y", delta))

    def router_3():
        here = place["y"]
        for m, delta in enumerate((1, 2, 3)):
            router_wait(4 + m, ref["rxy"].at[(here - delta) % 4])
        total = ref["rxy"][0] + ref["rxy"][1] + ref["rxy"][2] + ref["rxy"][3]
        ref["rxz"][z] = total
        for m, delta in enumerate((1, 2, 3)):
            router_send(7 + m, ref["rxz"].at[z], ref["rxz"].at[z], along("z", delta))

    def router_4():
        for m, delta in enumerate((1, 2, 3)):
            router_wait(7 + m, ref["rxz"].at[(z - delta) % 4])
        total = ref["rxz"][0] + ref["rxz"][1] + ref["rxz"][2] + ref["rxz"][3]
        for row in range(2):
            at = pl.ds(row, 1)
            fresh = adamw(total[:, row * 1024 : (row + 1) * 1024], *(part[at] for part in router_state))
            for part, value in zip(router_new, fresh):
                part[at] = value

    def router_sent():
        wait_send(ref["rx"], ref["r_send"].at[0])
        wait_send(ref["rxx"], ref["r_send"].at[1])
        wait_send(ref["rxy"].at[pl.ds(0, 3)], ref["r_send"].at[2])
        wait_send(ref["rxz"].at[pl.ds(0, 3)], ref["r_send"].at[3])

    router_stages = {0: router_0, 1: router_1, 2: router_2, 3: router_3, 4: router_4}

    def run(stage, *args):
        with jax.named_scope(f"{stage.__name__}#s={'_'.join(map(str, args)).replace(' ', '')}"):
            stage(*args)

    def live(step):
        return 0 <= step < STEPS

    def loaded(k):
        wait_recv(ref[f"grads0{k}"], ref["load_sem"].at[2 + k])
        wait_recv(ref[f"acts{k}"], ref["load_sem"].at[k])

    run(loaded, 0)
    small[0].wait()
    run(matmul, 0, 0, 8, (0,))
    run(loaded, 1)
    with jax.named_scope("barrier"):
        pl.semaphore_wait(barrier, len(peers))
    run(matmul, 0, 0, 8, (1,))
    run(add_sibling, 0)
    run(ring_start, 0, 1)

    def second(step):
        run(ring_end, step, 1)
        if step in DIRECT:
            run(second_start, step)
        else:
            run(ring_start, step, 2)
            run(ring_next, step, 2)

    def third(step):
        if step in DIRECT:
            run(second_end, step)
        else:
            run(ring_end, step, 2)
        run(last_start, step)

    def spread(step):
        run(last_end, step)
        ring_sent(step, 2)
        last_sent(step)
        if step in DIRECT_GATHER:
            run(gather_direct, step)
        else:
            run(gather_partner, step)

    def finish(step):
        run(gather_end, step)
        run(gather_sent, step)

    for i in range(STEPS):
        if live(i - 2):
            run(ring_relay, i - 2, 2)
        run(ring_next, i, 1)
        if i == 0:
            for copy in small[1:]:
                copy.wait()
            run(router_term)
            run(router_0)
            for k in range(2):
                wait_recv(ref[f"grads1{k}"], ref["load_sem"].at[4 + k])
            state_start()
        if live(i + 1):
            if live(i - 1):
                run(exchange_sent, i - 1)
            if live(i - 3):
                run(ring_sent, i - 3, 1)
            run(matmul, i + 1, 0, 4)
        if live(i - 1):
            second(i - 1)
        if live(i - 3):
            spread(i - 3)
        if live(i - 4):
            run(gather_start, i - 4)
        if live(i + 1):
            run(matmul, i + 1, 4, 8)
        run(ring_relay, i, 1)
        if live(i - 2):
            third(i - 2)
        if live(i + 1):
            run(add_sibling, i + 1)
            run(ring_start, i + 1, 1)
        if live(i - 4) and i < STEPS - 1:
            run(gather_relay, i - 4)
        if i + 1 in router_stages:
            run(router_stages[i + 1])
        if live(i - 5) and i < STEPS - 1:
            if i == 5:
                run(state_end)
            finish(i - 5)
    last = STEPS - 1
    run(ring_relay, last - 1, 2)
    run(gather_relay, last - 4)
    run(gather_start, last - 3)
    second(last)
    third(last - 1)
    spread(last - 2)
    run(gather_relay, last - 3)
    finish(last - 5)
    third(last)
    run(gather_start, last - 2)
    spread(last - 1)
    finish(last - 4)
    spread(last)
    run(gather_relay, last - 2)
    for step in (last - 3, last - 1, last, last - 2):
        finish(step)
    with jax.named_scope("ending"):
        for step in range(STEPS - 4, STEPS):
            if step >= STEPS - 2:
                exchange_sent(step)
            ring_sent(step, 1)
        router_sent()


def on_device(
    acts,
    grad_keys,
    grad_values,
    grad_logits,
    order,
    bucket_param,
    bucket_m,
    bucket_v,
    router_param,
    router_m,
    router_v,
):
    tree = scratch()
    names = tuple(tree)
    hbm, vmem = pl.BlockSpec(memory_space=pltpu.HBM), pl.BlockSpec(memory_space=pltpu.VMEM)
    fresh = pl.pallas_call(
        lambda *refs: kernel(names, *refs),
        out_shape=tuple(
            pltpu.VMEM(part.shape, F32) for part in (bucket_param, bucket_m, bucket_v, router_param, router_m, router_v)
        ),
        in_specs=[hbm] * 11,
        out_specs=(vmem,) * 6,
        scratch_shapes=list(tree.values()),
        compiler_params=pltpu.CompilerParams(
            collective_id=0, has_side_effects=True, vmem_limit_bytes=VMEM_LIMIT
        ),
        cost_estimate=pl.CostEstimate(flops=17_200_000_000, bytes_accessed=24_000_000, transcendentals=0),
        name="reduce",
    )(
        order,
        grad_logits,
        acts,
        grad_keys,
        grad_values,
        bucket_param,
        bucket_m,
        bucket_v,
        router_param,
        router_m,
        router_v,
    )
    return pl.pallas_call(
        store,
        out_shape=tuple(jax.ShapeDtypeStruct(part.shape, F32) for part in fresh),
        in_specs=[vmem] * 6,
        out_specs=(hbm,) * 6,
        scratch_shapes=[pltpu.SemaphoreType.DMA((15,))],
        compiler_params=pltpu.CompilerParams(vmem_limit_bytes=1024 * 1024),
        name="store",
    )(*(pltpu.with_memory_space_constraint(part, pltpu.VMEM) for part in fresh))


def store(*refs):
    copies = []
    for n in range(3):
        copies.append((refs[3 + n], refs[9 + n]))
        for b in range(BUCKETS):
            copies.append((refs[n].at[b], refs[6 + n].at[b]))
    copies = [pltpu.make_async_copy(src, dst, refs[12].at[n]) for n, (src, dst) in enumerate(copies)]
    for copy in copies:
        copy.start()
    for copy in copies:
        copy.wait()


def solution(mesh):
    state, router = P(None, "inst", None), P("inst", None)
    tokens = P(("rep", "inst"), None)
    return jax.shard_map(
        on_device,
        mesh=mesh,
        in_specs=(tokens, tokens, tokens, P(None, ("rep", "inst")), P(), state, state, state, router, router, router),
        out_specs=(state, state, state, router, router, router),
        check_vma=False,
    )
```
